32 devices in a mesh: dp: 1 (over z), tp: 4 (over y), ep: 8 (over x, core).
Axes of the slice: x: 4, y: 4, z: 1, core: 2. Of those that a mesh axis runs over, the one named last changes fastest.
The devices are a block of a 4x4x8 slice.
Arguments:
- x_in: bfloat16 [4096, 1024], P(('dp', 'ep', 'tp'))
- norm_gain: bfloat16 [1024], replicated
- w_router: bfloat16 [1024, 32], replicated
- expert_idx: int32 [4096, 8], P(('dp', 'ep', 'tp'))
- w_gate: bfloat16 [32, 1024, 512], P('ep', None, 'tp')
- w_up: bfloat16 [32, 1024, 512], P('ep', None, 'tp')
- w_down: bfloat16 [32, 512, 1024], P('ep', 'tp')
- out_bias: bfloat16 [1024], replicated
- dy_out: bfloat16 [4096, 1024], P(('dp', 'ep', 'tp'))
Outputs:
- output 1: bfloat16 [4096, 1024], P(('dp', 'ep', 'tp'))
- output 2: bfloat16 [4096, 1024], P(('dp', 'ep', 'tp'))
- output 3: float32 [1024], P('dp')
- output 4: float32 [1024, 32], P('dp')
- output 5: float32 [32, 1024, 512], P(('dp', 'ep'), None, 'tp')
- output 6: float32 [32, 1024, 512], P(('dp', 'ep'), None, 'tp')
- output 7: float32 [32, 512, 1024], P(('dp', 'ep'), 'tp')
- output 8: float32 [1024], P('dp')
All inputs are finite; a program needn't handle non-finite values.
Results may differ from the reference program's by a relative error of at most 0.0135311.
Values are sent between devices in bfloat16 or wider.
A program may use at most 768 MiB of HBM per device.

```python
import jax
import jax.numpy as jnp
from jax import lax

TOK = 128
D = 1024
FF = 512
EXPERTS = 32
TOP = 8
EP_DEVS = 8
TP_DEVS = 4
CAP = 64
EPS = 1e-6


def permute_tokens(perm_key):
    return jax.random.permutation(perm_key, TOK)


def draw_routing(route_key):
    n_src = EP_DEVS * TP_DEVS
    key_heavy, key_weight, key_perm = jax.random.split(route_key, 3)
    expert_row = jnp.arange(EXPERTS)[None, :]
    heavy = jax.random.randint(key_heavy, (n_src, 1), 0, EXPERTS)
    is_heavy = expert_row == heavy
    weights = jnp.where(is_heavy, 0, jax.random.randint(key_weight, (n_src, EXPERTS), 2, 5))
    rest = TOK * TOP - CAP
    share = rest * weights // jnp.sum(weights, axis=1, keepdims=True)
    left_over = rest - jnp.sum(share, axis=1, keepdims=True)
    light_rank = jnp.cumsum(jnp.where(is_heavy, 0, 1), axis=1) - 1
    extra = jnp.where(jnp.logical_and(jnp.logical_not(is_heavy), light_rank < left_over), 1, 0)
    counts = jnp.where(is_heavy, CAP, share + extra)
    ends = jnp.cumsum(counts, axis=1)
    position = jnp.arange(TOP)[None, :] * TOK + jnp.arange(TOK)[:, None]
    choice = jnp.sum((position[None, :, :, None] >= ends[:, None, None, :]).astype(jnp.int32), axis=-1)
    perms = jax.vmap(permute_tokens)(jax.random.split(key_perm, n_src))
    choice = jnp.take_along_axis(choice, perms[:, :, None], axis=1)
    return choice.reshape(n_src * TOK, TOP).astype(jnp.int32)


def setup_inputs(seed: int = 0, part: int = 0) -> dict:
    part_key = jax.random.fold_in(jax.random.key(seed), part)
    key_x, key_dy, key_route = jax.random.split(part_key, 3)
    key_g, key_r, key_wg, key_wu, key_wd, key_b = jax.random.split(jax.random.key(seed + 1), 6)
    n_rows = EP_DEVS * TP_DEVS * TOK
    x_in = jax.random.normal(key_x, (n_rows, D), jnp.float32).astype(jnp.bfloat16)
    norm_gain = (1.0 + 0.3 * jax.random.normal(key_g, (D,), jnp.float32)).astype(jnp.bfloat16)
    w_router = (2.0 * D ** -0.5 * jax.random.normal(key_r, (D, EXPERTS), jnp.float32)).astype(jnp.bfloat16)
    w_gate = (D ** -0.5 * jax.random.normal(key_wg, (EXPERTS, D, FF), jnp.float32)).astype(jnp.bfloat16)
    w_up = (D ** -0.5 * jax.random.normal(key_wu, (EXPERTS, D, FF), jnp.float32)).astype(jnp.bfloat16)
    w_down = (1.5 * FF ** -0.5 * jax.random.normal(key_wd, (EXPERTS, FF, D), jnp.float32)).astype(jnp.bfloat16)
    out_bias = (0.5 * jax.random.normal(key_b, (D,), jnp.float32)).astype(jnp.bfloat16)
    dy_out = jax.random.normal(key_dy, (n_rows, D), jnp.float32).astype(jnp.bfloat16)
    expert_idx = draw_routing(key_route)
    return {"x_in": x_in, "norm_gain": norm_gain, "w_router": w_router, "expert_idx": expert_idx, "w_gate": w_gate, "w_up": w_up, "w_down": w_down, "out_bias": out_bias, "dy_out": dy_out}


def to_bf16(values):
    return values + lax.stop_gradient(values.astype(jnp.bfloat16).astype(jnp.float32) - values)


def reference(x_in, norm_gain, w_router, expert_idx, w_gate, w_up, w_down, out_bias, dy_out):
    n_rows = x_in.shape[0]
    rows_max = EP_DEVS * TP_DEVS * CAP
    flat_ids = expert_idx.reshape(-1)
    order = jnp.argsort(flat_ids, stable=True)
    counts = jnp.sum((flat_ids[:, None] == jnp.arange(EXPERTS)[None, :]).astype(jnp.int32), axis=0)
    starts = jnp.cumsum(counts) - counts
    slot_rank = jnp.arange(rows_max)[None, :]
    slot_tok = order[jnp.minimum(starts[:, None] + slot_rank, n_rows * TOP - 1)] // TOP
    slot_ok = slot_rank < counts[:, None]
    copy_pos = (flat_ids * rows_max + jnp.argsort(order) - starts[flat_ids]).reshape(n_rows, TOP)

    def forward(x_f32, gain, router, gate_w, up_w, down_w, bias):
        inv_rms = lax.rsqrt(jnp.mean(x_f32 * x_f32, axis=-1, keepdims=True) + EPS)
        hidden = to_bf16(x_f32 * inv_rms * gain)
        logits = jnp.dot(hidden, router, preferred_element_type=jnp.float32)
        gates = jax.nn.softmax(jnp.take_along_axis(logits, expert_idx, axis=1), axis=-1)

        def one_expert(operands):
            gate_e, up_e, down_e, tok_e, ok_e = operands
            rows_in = jnp.where(ok_e[:, None], hidden[tok_e], 0.0)
            gate_pre = jnp.dot(rows_in, gate_e, preferred_element_type=jnp.float32)
            up_pre = jnp.dot(rows_in, up_e, preferred_element_type=jnp.float32)
            hidden_act = to_bf16(jax.nn.silu(gate_pre) * up_pre)
            return to_bf16(jnp.dot(hidden_act, down_e, preferred_element_type=jnp.float32))

        y_slots = lax.map(jax.checkpoint(one_expert), (gate_w, up_w, down_w, slot_tok, slot_ok))
        y_copy = y_slots.reshape(EXPERTS * rows_max, D)[copy_pos]
        return x_f32 + jnp.sum(gates[:, :, None] * y_copy, axis=1) + bias

    y_f32, pullback = jax.vjp(forward, x_in.astype(jnp.float32), norm_gain.astype(jnp.float32), w_router.astype(jnp.float32), w_gate.astype(jnp.float32), w_up.astype(jnp.float32), w_down.astype(jnp.float32), out_bias.astype(jnp.float32))
    cotangents = pullback(dy_out.astype(jnp.float32))
    return (y_f32.astype(jnp.bfloat16), cotangents[0].astype(jnp.bfloat16), cotangents[1], cotangents[2], cotangents[3], cotangents[4], cotangents[5], cotangents[6])
```

```python
import jax
import jax.numpy as jnp
from jax import lax
from jax.experimental import pallas as pl
from jax.experimental.pallas import tpu as pltpu
from jax.sharding import PartitionSpec as P

EPS = 1e-6
MESH = pl.DeviceIdType.MESH
F32 = jnp.float32
BF16 = jnp.bfloat16
ORDER = ((0, 0), (1, 0), (3, 0), (0, 1), (0, 3), (2, 0), (0, 2), (1, 1), (1, 3), (1, 2), (3, 1), (3, 3), (3, 2), (2, 1), (2, 3), (2, 2))
SLOT = {place: k for k, place in enumerate(ORDER)}
N_SLOT = len(ORDER)
N_SEND = 67
LAG = 2


def dot_nt(a, b):
    return lax.dot_general(a, b, (((1,), (1,)), ((), ())), preferred_element_type=F32)


def moe_kernel(h_ref, dy_ref, gate_ref, wg_ref, wu_ref, wd_ref,
               ysum_ref, dhsum_ref, dgate_ref, dbias_ref, dwg_ref, dwu_ref, dwd_ref,
               x_own, x_sib, part, g_own, g_sib, pg_own, pg_sib, q_buf, qg_buf,
               r1, r1g, r2, r2g, r3, r3g, r4, r4g, wgu, wd, acc_gu, acc_d, acc_b,
               load_sem, ag_send, ag_recv, ag_grecv, sib_recv,
               rq_send, rq_recv, s1_send, s1_recv, s2_send, s2_recv, f1_send, f1_recv, f2_send, f2_recv):
    ep = lax.axis_index("ep")
    tp = lax.axis_index("tp")
    n_tp = lax.axis_size("tp")
    n_x = lax.axis_size("ep") // 2
    core = lax.rem(ep, 2)
    chip_x = lax.div(ep, 2)
    n_loc, d_model, width = wg_ref.shape
    n_tok = h_ref.shape[0]
    n_exp = gate_ref.shape[0]
    loc = n_loc * width

    def shifted(x_step, y_step):
        x_new = lax.rem(chip_x + x_step + n_x, n_x)
        y_new = lax.rem(tp + y_step + n_tp, n_tp)
        return {"tp": y_new, "ep": 2 * x_new + core}

    f_up = shifted(1 - core, core)
    f_dn = shifted(core - 1, -core)
    s_up = shifted(core, 1 - core)
    s_dn = shifted(-core, core - 1)
    sib = {"ep": ep + 1 - 2 * core}

    loads = []
    for e in range(n_loc):
        cols = pl.ds(e * width, width)
        loads.append(pltpu.make_async_copy(wg_ref.at[e], wgu.at[:, cols], load_sem.at[len(loads)]))
        loads.append(pltpu.make_async_copy(wu_ref.at[e], wgu.at[:, pl.ds(loc + e * width, width)], load_sem.at[len(loads)]))
        loads.append(pltpu.make_async_copy(wd_ref.at[e], wd.at[cols], load_sem.at[len(loads)]))
    for c in loads:
        c.start()
    x_own[0, 0] = h_ref[...]
    x_own[0, 1] = dy_ref[...]
    g_own[0] = gate_ref[...]

    barrier = pltpu.get_barrier_semaphore()
    for dev in (f_up, f_dn, s_up, s_dn, sib):
        pl.semaphore_signal(barrier, inc=1, device_id=dev, device_id_type=MESH)
    pl.semaphore_wait(barrier, 5)

    def remote(src, dst, send, recv, dev):
        return pltpu.make_async_remote_copy(src_ref=src, dst_ref=dst, send_sem=send, recv_sem=recv, device_id=dev, device_id_type=MESH)

    sends = {k: [] for k in range(N_SLOT)}
    count = [0]

    def plan(k, src, dst, recv, dev):
        n = count[0]
        count[0] += 1
        sends[k].append(lambda: remote(src, dst, ag_send.at[n], recv, dev))

    def plan_block(k, to, dev):
        plan(k, x_own.at[k], x_own.at[to], ag_recv.at[to, 0], dev)
        plan(k, g_own.at[k], g_own.at[to], ag_grecv.at[to], dev)

    plan_block(0, SLOT[(3, 0)], f_up)
    plan_block(0, SLOT[(1, 0)], f_dn)
    for k, (df, ds) in enumerate(ORDER):
        if (df, ds) == (3, 0):
            to = SLOT[(2, 0)]
            plan(k, x_own.at[k, 0], x_own.at[to, 0], ag_recv.at[to, 0], f_up)
            plan(k, g_own.at[k], g_own.at[to], ag_grecv.at[to], f_up)
        if (df, ds) == (1, 0):
            to = SLOT[(2, 0)]
            plan(k, x_own.at[k, 1], x_own.at[to, 1], ag_recv.at[to, 1], f_dn)
        if ds == 0:
            plan_block(k, SLOT[(df, 3)], s_up)
            plan_block(k, SLOT[(df, 1)], s_dn)
        if ds == 3:
            to = SLOT[(df, 2)]
            plan(k, x_own.at[k, 0], x_own.at[to, 0], ag_recv.at[to, 0], s_up)
            plan(k, g_own.at[k], g_own.at[to], ag_grecv.at[to], s_up)
        if ds == 1:
            to = SLOT[(df, 2)]
            plan(k, x_own.at[k, 1], x_own.at[to, 1], ag_recv.at[to, 1], s_dn)
        plan(k, x_own.at[k], x_sib.at[k], sib_recv.at[k, 0], sib)
        plan(k, g_own.at[k], g_sib.at[k], sib_recv.at[k, 1], sib)
    assert count[0] == N_SEND

    def arrive(k):
        if k:
            if ORDER[k][1] == 2 or ORDER[k] == (2, 0):
                for t in range(2):
                    remote(x_own.at[k, t], x_own.at[k, t], ag_send.at[0], ag_recv.at[k, t], sib).wait_recv()
            else:
                remote(x_own.at[k], x_own.at[k], ag_send.at[0], ag_recv.at[k, 0], sib).wait_recv()
            remote(g_own.at[k], g_own.at[k], ag_send.at[0], ag_grecv.at[k], sib).wait_recv()
        for make in sends[k]:
            make().start()

    def to_sibling(k):
        return (remote(x_sib.at[k], q_buf.at[k], rq_send.at[k, 0], rq_recv.at[k, 0], sib),
                remote(pg_sib.at[k], qg_buf.at[k], rq_send.at[k, 1], rq_recv.at[k, 1], sib))

    def add_sibling(k):
        for c in to_sibling(k):
            c.wait_recv()
        part[k] = (part[k].astype(F32) + q_buf[k].astype(F32)).astype(BF16)
        pg_own[k] = pg_own[k] + qg_buf[k]

    def s_first(df):
        k = SLOT[(df, 2)]
        return (remote(part.at[k, 0], r1.at[df, 0], s1_send.at[df, 0], s1_recv.at[df, 0], s_up),
                remote(part.at[k, 1], r1.at[df, 1], s1_send.at[df, 1], s1_recv.at[df, 1], s_dn),
                remote(pg_own.at[k], r1g.at[df], s1_send.at[df, 2], s1_recv.at[df, 2], s_up))

    row = lax.broadcasted_iota(jnp.int32, (n_exp, loc), 0)
    col = lax.broadcasted_iota(jnp.int32, (n_exp, loc), 1)
    pick = jnp.where(row == ep * n_loc + lax.div(col, width), 1.0, 0.0).astype(F32)

    def widen(g):
        return lax.dot_general(g, pick, (((0,), (0,)), ((), ())), precision=lax.Precision.HIGHEST, preferred_element_type=F32)

    def compute(k):
        h = jnp.concatenate([x_own[k, 0], x_sib[k, 0]], axis=0)
        dy = jnp.concatenate([x_own[k, 1], x_sib[k, 1]], axis=0)
        gate = jnp.concatenate([widen(g_own[k]), widen(g_sib[k])], axis=0)
        both = jnp.dot(h, wgu[...], preferred_element_type=F32)
        g_pre = both[:, :loc]
        u_pre = both[:, loc:]
        d_raw = dot_nt(dy, wd[...])
        used = gate != 0.0
        sig = jax.nn.sigmoid(g_pre)
        silu = g_pre * sig
        act = (silu * u_pre).astype(BF16).astype(F32)
        act_g = jnp.where(used, gate * act, 0.0).astype(BF16)
        prod = jnp.where(used, act * d_raw, 0.0)
        d_act = gate * d_raw
        d_g = jnp.where(used, d_act * u_pre * sig * (1.0 + g_pre * (1.0 - sig)), 0.0).astype(BF16)
        d_u = jnp.where(used, d_act * silu, 0.0).astype(BF16)
        d_gu = jnp.concatenate([d_g, d_u], axis=1)
        prod_hi = prod.astype(BF16)
        prod_lo = (prod - prod_hi.astype(F32)).astype(BF16)
        pick_b = pick.astype(BF16)
        dgate = dot_nt(pick_b, prod_hi) + dot_nt(pick_b, prod_lo)
        pg_own[k] = dgate[:, :n_tok]
        pg_sib[k] = dgate[:, n_tok:]
        acc_b[...] += jnp.sum(dy.astype(F32).reshape(2 * n_tok // 8, 8, d_model), axis=0)
        acc_gu[...] += jnp.dot(h.T, d_gu, preferred_element_type=F32)
        acc_d[...] += jnp.dot(act_g.T, dy, preferred_element_type=F32)
        y = jnp.dot(act_g, wd[...], preferred_element_type=F32).astype(BF16)
        part[k, 0] = y[:n_tok]
        x_sib[k, 0] = y[n_tok:]
        dh = dot_nt(d_gu, wgu[...]).astype(BF16)
        part[k, 1] = dh[:n_tok]
        x_sib[k, 1] = dh[n_tok:]

    arrive(0)
    acc_gu[...] = jnp.zeros_like(acc_gu)
    acc_d[...] = jnp.zeros_like(acc_d)
    acc_b[...] = jnp.zeros_like(acc_b)
    for c in loads:
        c.wait()

    def step(k, carry):
        for j in range(N_SLOT - 1):
            @pl.when(k == j)
            def _():
                arrive(j + 1)
        remote(x_own.at[k], x_sib.at[k], ag_send.at[0], sib_recv.at[k, 0], sib).wait_recv()
        remote(g_own.at[k], g_sib.at[k], ag_send.at[0], sib_recv.at[k, 1], sib).wait_recv()
        compute(k)
        for c in to_sibling(k):
            c.start()

        @pl.when(k >= LAG)
        def _():
            add_sibling(k - LAG)
        for j, (df, ds) in enumerate(ORDER[:N_SLOT - LAG]):
            if ds == 2:
                @pl.when(k == j + LAG)
                def _():
                    for c in s_first(df):
                        c.start()
        return carry

    lax.fori_loop(0, N_SLOT, step, 0)

    stores = []
    for e in range(n_loc):
        cols = pl.ds(e * width, width)
        stores.append(pltpu.make_async_copy(acc_gu.at[:, cols], dwg_ref.at[e], load_sem.at[len(stores)]))
        stores.append(pltpu.make_async_copy(acc_gu.at[:, pl.ds(loc + e * width, width)], dwu_ref.at[e], load_sem.at[len(stores)]))
        stores.append(pltpu.make_async_copy(acc_d.at[cols], dwd_ref.at[e], load_sem.at[len(stores)]))
    for c in stores:
        c.start()
    dbias_ref[...] = acc_b[...]

    for j in range(N_SLOT - LAG, N_SLOT):
        add_sibling(j)
        df, ds = ORDER[j]
        if ds == 2:
            for c in s_first(df):
                c.start()

    def s_second(df, i):
        k = SLOT[(df, (1, 3)[i])]
        dev = (s_up, s_dn)[i]
        return (remote(part.at[k], r2.at[df, i], s2_send.at[df, i, 0], s2_recv.at[df, i, 0], dev),
                remote(pg_own.at[k], r2g.at[df, i], s2_send.at[df, i, 1], s2_recv.at[df, i, 1], dev))

    def add_into(k, t, block):
        part[k, t] = (part[k, t].astype(F32) + block[...].astype(F32)).astype(BF16)

    for df in (0, 1, 3, 2):
        for c in s_first(df):
            c.wait_recv()
        k = SLOT[(df, 1)]
        add_into(k, 0, r1.at[df, 0])
        pg_own[k] = pg_own[k] + r1g[df]
        add_into(SLOT[(df, 3)], 1, r1.at[df, 1])
        for i in range(2):
            for c in s_second(df, i):
                c.start()

    k2, k1, k3 = SLOT[(2, 0)], SLOT[(1, 0)], SLOT[(3, 0)]

    def wait_second(df):
        for i in range(2):
            for c in s_second(df, i):
                c.wait_recv()
        pg_own[SLOT[(df, 0)]] = pg_own[SLOT[(df, 0)]] + r2g[df, 0] + r2g[df, 1]

    def total(k, df, t):
        return part[k, t].astype(F32) + r2[df, 0, t].astype(F32) + r2[df, 1, t].astype(F32)

    f_first = (remote(part.at[k2, 0], r3.at[0], f1_send.at[0], f1_recv.at[0], f_up),
               remote(part.at[k2, 1], r3.at[1], f1_send.at[1], f1_recv.at[1], f_dn),
               remote(pg_own.at[k2], r3g, f1_send.at[2], f1_recv.at[2], f_up))
    f_second = (remote(part.at[k1], r4.at[0], f2_send.at[0], f2_recv.at[0], f_up),
                remote(pg_own.at[k1], r4g.at[0], f2_send.at[1], f2_recv.at[1], f_up),
                remote(part.at[k3], r4.at[1], f2_send.at[2], f2_recv.at[2], f_dn),
                remote(pg_own.at[k3], r4g.at[1], f2_send.at[3], f2_recv.at[3], f_dn))
    wait_second(1)
    part[k1, 0] = total(k1, 1, 0).astype(BF16)
    part[k1, 1] = total(k1, 1, 1).astype(BF16)
    wait_second(3)
    part[k3, 0] = total(k3, 3, 0).astype(BF16)
    part[k3, 1] = total(k3, 3, 1).astype(BF16)
    wait_second(0)
    ysum_ref[...] = total(0, 0, 0)
    dhsum_ref[...] = total(0, 0, 1)
    wait_second(2)
    part[k2, 0] = total(k2, 2, 0).astype(BF16)
    part[k2, 1] = total(k2, 2, 1).astype(BF16)
    for c in f_first:
        c.start()
    for c in f_first:
        c.wait_recv()
    add_into(k1, 0, r3.at[0])
    pg_own[k1] = pg_own[k1] + r3g[...]
    add_into(k3, 1, r3.at[1])
    for c in f_second:
        c.start()
    for c in f_second:
        c.wait_recv()
    ysum_ref[...] = ysum_ref[...] + r4[0, 0].astype(F32) + r4[1, 0].astype(F32)
    dhsum_ref[...] = dhsum_ref[...] + r4[0, 1].astype(F32) + r4[1, 1].astype(F32)
    dgate_ref[...] = pg_own[0] + r4g[0] + r4g[1]

    for c in stores:
        c.wait()
    for k in range(N_SLOT):
        for make in sends[k]:
            make().wait_send()
        for c in to_sibling(k):
            c.wait_send()
    for df in range(4):
        for c in s_first(df):
            c.wait_send()
        for i in range(2):
            for c in s_second(df, i):
                c.wait_send()
    for c in f_first + f_second:
        c.wait_send()


def moe(h, dy, gate_t, w_gate, w_up, w_down):
    n_tok, d_model = h.shape
    n_loc, _, width = w_gate.shape
    n_exp = gate_t.shape[0]
    loc = n_loc * width
    vmem = pl.BlockSpec(memory_space=pltpu.VMEM)
    hbm = pl.BlockSpec(memory_space=pl.ANY)
    block = (2, n_tok, d_model)
    small = (n_exp, n_tok)
    dma = pltpu.SemaphoreType.DMA
    scratch = [
        pltpu.VMEM((N_SLOT, *block), BF16), pltpu.VMEM((N_SLOT, *block), BF16), pltpu.VMEM((N_SLOT, *block), BF16),
        pltpu.VMEM((N_SLOT, *small), F32), pltpu.VMEM((N_SLOT, *small), F32),
        pltpu.VMEM((N_SLOT, *small), F32), pltpu.VMEM((N_SLOT, *small), F32),
        pltpu.VMEM((N_SLOT, *block), BF16), pltpu.VMEM((N_SLOT, *small), F32),
        pltpu.VMEM((4, *block), BF16), pltpu.VMEM((4, *small), F32),
        pltpu.VMEM((4, 2, *block), BF16), pltpu.VMEM((4, 2, *small), F32),
        pltpu.VMEM(block, BF16), pltpu.VMEM(small, F32),
        pltpu.VMEM((2, *block), BF16), pltpu.VMEM((2, *small), F32),
        pltpu.VMEM((d_model, 2 * loc), BF16), pltpu.VMEM((loc, d_model), BF16),
        pltpu.VMEM((d_model, 2 * loc), F32), pltpu.VMEM((loc, d_model), F32), pltpu.VMEM((8, d_model), F32),
        dma((3 * n_loc,)), dma((N_SEND,)), dma((N_SLOT, 2)), dma((N_SLOT,)), dma((N_SLOT, 2)),
        dma((N_SLOT, 2)), dma((N_SLOT, 2)), dma((4, 3)), dma((4, 3)), dma((4, 2, 2)), dma((4, 2, 2)),
        dma((3,)), dma((3,)), dma((4,)), dma((4,)),
    ]
    out_shape = (
        jax.ShapeDtypeStruct((n_tok, d_model), F32), jax.ShapeDtypeStruct((n_tok, d_model), F32),
        jax.ShapeDtypeStruct(small, F32), jax.ShapeDtypeStruct((8, d_model), F32),
        jax.ShapeDtypeStruct(w_gate.shape, F32), jax.ShapeDtypeStruct(w_up.shape, F32), jax.ShapeDtypeStruct(w_down.shape, F32),
    )
    return pl.pallas_call(
        moe_kernel, name="moe", out_shape=out_shape,
        in_specs=[vmem, vmem, vmem, hbm, hbm, hbm], out_specs=(vmem, vmem, vmem, vmem, hbm, hbm, hbm),
        scratch_shapes=scratch,
        compiler_params=pltpu.CompilerParams(collective_id=0, has_side_effects=True, vmem_limit_bytes=67_043_328),
    )(h, dy, gate_t, w_gate, w_up, w_down)


def solution(mesh):
    tok_spec = P(("dp", "ep", "tp"), None)
    wide_spec = P("ep", None, "tp")
    down_spec = P("ep", "tp", None)
    grad_wide = P(("dp", "ep"), None, "tp")
    grad_down = P(("dp", "ep"), "tp", None)

    def device_step(x_in, norm_gain, w_router, expert_idx, w_gate, w_up, w_down, out_bias, dy_out):
        n_exp = w_router.shape[1]
        x_f32 = x_in.astype(F32)
        inv_rms = lax.rsqrt(jnp.mean(x_f32 * x_f32, axis=-1, keepdims=True) + EPS)
        normed = x_f32 * inv_rms
        gain_f32 = norm_gain.astype(F32)
        hidden = (normed * gain_f32).astype(BF16)
        logits = jnp.dot(hidden, w_router, preferred_element_type=F32)
        chosen = jnp.any(expert_idx[:, :, None] == jnp.arange(n_exp)[None, None, :], axis=1)
        gates = jax.nn.softmax(jnp.where(chosen, logits, -jnp.inf), axis=-1)
        y_sum, dh_sum, dgate_t, dbias_8, d_gate, d_up, d_down = moe(hidden, dy_out, gates.T, w_gate, w_up, w_down)
        d_gates = jnp.where(chosen, dgate_t.T, 0.0)
        y_out = (x_f32 + (y_sum + out_bias.astype(F32))).astype(BF16)
        dy_f32 = dy_out.astype(F32)
        d_logits = gates * (d_gates - jnp.sum(gates * d_gates, axis=-1, keepdims=True))
        d_router = jnp.einsum("td,te->de", hidden, d_logits, preferred_element_type=F32)
        dh_total = dh_sum + jnp.einsum("te,de->td", d_logits, w_router, preferred_element_type=F32)
        d_gain = jnp.sum(dh_total * normed, axis=0)
        d_norm = dh_total * gain_f32
        dx_in = (dy_f32 + inv_rms * (d_norm - normed * jnp.mean(d_norm * normed, axis=-1, keepdims=True))).astype(BF16)
        d_gain, d_router = lax.psum((d_gain, d_router), ("ep", "tp"))
        return y_out, dx_in, d_gain, d_router, d_gate, d_up, d_down, jnp.sum(dbias_8, axis=0)

    return jax.shard_map(device_step, mesh=mesh, in_specs=(tok_spec, P(None), P(None, None), tok_spec, wide_spec, wide_spec, down_spec, P(None), tok_spec), out_specs=(tok_spec, tok_spec, P("dp"), P("dp", None), grad_wide, grad_wide, grad_down, P("dp")), check_vma=False)
```

```python
import jax
import jax.numpy as jnp
from jax import lax
from jax.experimental import pallas as pl
from jax.experimental.pallas import tpu as pltpu
from jax.sharding import PartitionSpec as P

EPS = 1e-6
MESH = pl.DeviceIdType.MESH
F32 = jnp.float32
BF16 = jnp.bfloat16
ORDER = ((0, 0), (0, 1), (0, 3), (0, 2), (1, 0), (1, 1), (1, 3), (3, 1), (3, 3), (1, 2), (2, 1), (2, 3), (3, 2), (2, 2), (2, 0), (3, 0))
ARRIVALS = {1: ((0, 1), (0, 3), (1, 0), (3, 0)), 2: ((2, 0), (0, 2)), 4: ((1, 1), (1, 3)), 6: ((3, 1), (3, 3)),
            8: ((1, 2),), 9: ((2, 1), (2, 3)), 11: ((3, 2),), 12: ((2, 2),)}
FIRST_AT = {4: 0, 10: 1, 13: 3, 14: 2}
SECOND_AT = {6: 0, 12: 1, 15: 3}
SLOT = {place: k for k, place in enumerate(ORDER)}
N_SLOT = len(ORDER)
N_SEND = 67
LAG = 1


def dot_nt(a, b):
    return lax.dot_general(a, b, (((1,), (1,)), ((), ())), preferred_element_type=F32)


def moe_kernel(x_ref, dy_ref, idx_ref, gain_ref, bias_ref, router_ref, wg_ref, wu_ref, wd_ref,
               y_ref, dx_ref, dgain_ref, drouter_ref, dbias_ref, dwg_ref, dwu_ref, dwd_ref,
               x_own, x_sib, part, g_own, g_sib, pg_own, pg_sib, q_buf, qg_buf,
               r1, r1g, r2, r2g, r3, r3g, r4, r4g, dl_buf, dr_buf, gn_buf, wgu, wd, acc_gu, acc_d, acc_b,
               load_sem, ag_send, ag_recv, ag_grecv, sib_recv,
               rq_send, rq_recv, s1_send, s1_recv, s2_send, s2_recv, f1_send, f1_recv, f2_send, f2_recv, e_send, e_recv):
    ep = lax.axis_index("ep")
    tp = lax.axis_index("tp")
    n_tp = lax.axis_size("tp")
    n_x = lax.axis_size("ep") // 2
    core = lax.rem(ep, 2)
    chip_x = lax.div(ep, 2)
    n_loc, d_model, width = wg_ref.shape
    n_tok = x_ref.shape[0]
    n_exp = router_ref.shape[0]
    loc = n_loc * width

    def shifted(x_step, y_step):
        x_new = lax.rem(chip_x + x_step + n_x, n_x)
        y_new = lax.rem(tp + y_step + n_tp, n_tp)
        return {"tp": y_new, "ep": 2 * x_new + core}

    f_up = shifted(1 - core, core)
    f_dn = shifted(core - 1, -core)
    s_up = shifted(core, 1 - core)
    s_dn = shifted(-core, core - 1)
    f_op = shifted(2 * (1 - core), 2 * core)
    s_op = shifted(2 * core, 2 * (1 - core))
    sib = {"ep": ep + 1 - 2 * core}

    loads = []
    for e in range(n_loc):
        cols = pl.ds(e * width, width)
        loads.append(pltpu.make_async_copy(wg_ref.at[e], wgu.at[:, cols], load_sem.at[len(loads)]))
        loads.append(pltpu.make_async_copy(wu_ref.at[e], wgu.at[:, pl.ds(loc + e * width, width)], load_sem.at[len(loads)]))
        loads.append(pltpu.make_async_copy(wd_ref.at[e], wd.at[cols], load_sem.at[len(loads)]))
    for c in loads:
        c.start()
    barrier = pltpu.get_barrier_semaphore()
    peers = (f_up, f_dn, f_op, s_up, s_dn, s_op, sib)
    for dev in peers:
        pl.semaphore_signal(barrier, inc=1, device_id=dev, device_id_type=MESH)

    def normalised():
        x = x_ref[...].astype(F32)
        inv_rms = lax.rsqrt(jnp.mean(x * x, axis=-1, keepdims=True) + EPS)
        return x, inv_rms, x * inv_rms

    def chosen_mask():
        expert = lax.broadcasted_iota(jnp.int32, (n_exp, n_tok), 0)
        chosen = expert == idx_ref[0:1, :]
        for j in range(1, idx_ref.shape[0]):
            chosen = jnp.logical_or(chosen, expert == idx_ref[j:j + 1, :])
        return chosen

    gain = gain_ref[...].astype(F32)
    hidden = (normalised()[2] * gain).astype(BF16)
    x_own[0, 0] = hidden
    x_own[0, 1] = dy_ref[...]
    logits = jnp.where(chosen_mask(), dot_nt(router_ref[...], hidden), -jnp.inf)
    weight = jnp.exp(logits - jnp.max(logits, axis=0, keepdims=True))
    g_own[0] = weight / jnp.sum(weight, axis=0, keepdims=True)
    pl.semaphore_wait(barrier, len(peers))

    def remote(src, dst, send, recv, dev):
        return pltpu.make_async_remote_copy(src_ref=src, dst_ref=dst, send_sem=send, recv_sem=recv, device_id=dev, device_id_type=MESH)

    sends = {k: [] for k in range(N_SLOT)}
    count = [0]

    def plan(k, src, dst, recv, dev):
        n = count[0]
        count[0] += 1
        sends[k].append(lambda: remote(src, dst, ag_send.at[n], recv, dev))

    def plan_block(k, to, dev):
        plan(k, x_own.at[k], x_own.at[to], ag_recv.at[to, 0], dev)
        plan(k, g_own.at[k], g_own.at[to], ag_grecv.at[to], dev)

    plan_block(0, SLOT[(3, 0)], f_up)
    plan_block(0, SLOT[(1, 0)], f_dn)
    for k, (df, ds) in enumerate(ORDER):
        if (df, ds) == (3, 0):
            to = SLOT[(2, 0)]
            plan(k, x_own.at[k, 0], x_own.at[to, 0], ag_recv.at[to, 0], f_up)
            plan(k, g_own.at[k], g_own.at[to], ag_grecv.at[to], f_up)
        if (df, ds) == (1, 0):
            to = SLOT[(2, 0)]
            plan(k, x_own.at[k, 1], x_own.at[to, 1], ag_recv.at[to, 1], f_dn)
        if ds == 0:
            plan_block(k, SLOT[(df, 3)], s_up)
            plan_block(k, SLOT[(df, 1)], s_dn)
        if ds == 3:
            to = SLOT[(df, 2)]
            plan(k, x_own.at[k, 0], x_own.at[to, 0], ag_recv.at[to, 0], s_up)
            plan(k, g_own.at[k], g_own.at[to], ag_grecv.at[to], s_up)
        if ds == 1:
            to = SLOT[(df, 2)]
            plan(k, x_own.at[k, 1], x_own.at[to, 1], ag_recv.at[to, 1], s_dn)
        plan(k, x_own.at[k], x_sib.at[k], sib_recv.at[k, 0], sib)
        plan(k, g_own.at[k], g_sib.at[k], sib_recv.at[k, 1], sib)
    assert count[0] == N_SEND

    def arrive(k):
        if k:
            if ORDER[k][1] == 2 or ORDER[k] == (2, 0):
                for t in range(2):
                    remote(x_own.at[k, t], x_own.at[k, t], ag_send.at[0], ag_recv.at[k, t], sib).wait_recv()
            else:
                remote(x_own.at[k], x_own.at[k], ag_send.at[0], ag_recv.at[k, 0], sib).wait_recv()
            remote(g_own.at[k], g_own.at[k], ag_send.at[0], ag_grecv.at[k], sib).wait_recv()
        for make in sends[k]:
            make().start()

    def to_sibling(k):
        return (remote(x_sib.at[k], q_buf.at[k], rq_send.at[k, 0], rq_recv.at[k, 0], sib),
                remote(pg_sib.at[k], qg_buf.at[k], rq_send.at[k, 1], rq_recv.at[k, 1], sib))

    def add_sibling(k):
        for c in to_sibling(k):
            c.wait_recv()
        part[k] = (part[k].astype(F32) + q_buf[k].astype(F32)).astype(BF16)
        pg_own[k] = pg_own[k] + qg_buf[k]

    def s_first(df):
        k = SLOT[(df, 2)]
        return (remote(part.at[k, 0], r1.at[df, 0], s1_send.at[df, 0], s1_recv.at[df, 0], s_up),
                remote(part.at[k, 1], r1.at[df, 1], s1_send.at[df, 1], s1_recv.at[df, 1], s_dn),
                remote(pg_own.at[k], r1g.at[df], s1_send.at[df, 2], s1_recv.at[df, 2], s_up))

    def s_second(df, i):
        k = SLOT[(df, (1, 3)[i])]
        dev = (s_up, s_dn)[i]
        return (remote(pg_own.at[k], r2g.at[df, i], s2_send.at[df, i, 1], s2_recv.at[df, i, 1], dev),
                remote(part.at[k], r2.at[df, i], s2_send.at[df, i, 0], s2_recv.at[df, i, 0], dev))

    def add_into(k, t, block):
        part[k, t] = (part[k, t].astype(F32) + block[...].astype(F32)).astype(BF16)

    def send_second(df):
        for c in s_first(df):
            c.wait_recv()
        k = SLOT[(df, 1)]
        add_into(k, 0, r1.at[df, 0])
        pg_own[k] = pg_own[k] + r1g[df]
        add_into(SLOT[(df, 3)], 1, r1.at[df, 1])
        for i in range(2):
            for c in s_second(df, i):
                c.start()

    row = lax.broadcasted_iota(jnp.int32, (n_exp, loc), 0)
    col = lax.broadcasted_iota(jnp.int32, (n_exp, loc), 1)
    pick = jnp.where(row == ep * n_loc + lax.div(col, width), 1.0, 0.0).astype(F32)

    def widen(g):
        return lax.dot_general(g, pick, (((0,), (0,)), ((), ())), precision=lax.Precision.HIGHEST, preferred_element_type=F32)

    def compute(k):
        h = jnp.concatenate([x_own[k, 0], x_sib[k, 0]], axis=0)
        dy = jnp.concatenate([x_own[k, 1], x_sib[k, 1]], axis=0)
        gate = jnp.concatenate([widen(g_own[k]), widen(g_sib[k])], axis=0)
        both = jnp.dot(h, wgu[...], preferred_element_type=F32)
        g_pre = both[:, :loc]
        u_pre = both[:, loc:]
        d_raw = dot_nt(dy, wd[...])
        used = gate != 0.0
        sig = jax.nn.sigmoid(g_pre)
        silu = g_pre * sig
        act = (silu * u_pre).astype(BF16).astype(F32)
        act_g = jnp.where(used, gate * act, 0.0).astype(BF16)
        prod = jnp.where(used, act * d_raw, 0.0)
        d_act = gate * d_raw
        d_g = jnp.where(used, d_act * u_pre * sig * (1.0 + g_pre * (1.0 - sig)), 0.0).astype(BF16)
        d_u = jnp.where(used, d_act * silu, 0.0).astype(BF16)
        d_gu = jnp.concatenate([d_g, d_u], axis=1)
        prod_hi = prod.astype(BF16)
        prod_lo = (prod - prod_hi.astype(F32)).astype(BF16)
        pick_b = pick.astype(BF16)
        dgate = dot_nt(pick_b, prod_hi) + dot_nt(pick_b, prod_lo)
        pg_own[k] = dgate[:, :n_tok]
        pg_sib[k] = dgate[:, n_tok:]
        acc_b[...] += jnp.sum(dy.astype(F32).reshape(2 * n_tok // 8, 8, d_model), axis=0)
        acc_gu[...] += jnp.dot(h.T, d_gu, preferred_element_type=F32)
        acc_d[...] += jnp.dot(act_g.T, dy, preferred_element_type=F32)
        y = jnp.dot(act_g, wd[...], preferred_element_type=F32).astype(BF16)
        part[k, 0] = y[:n_tok]
        x_sib[k, 0] = y[n_tok:]
        dh = dot_nt(d_gu, wgu[...]).astype(BF16)
        part[k, 1] = dh[:n_tok]
        x_sib[k, 1] = dh[n_tok:]

    arrive(0)
    acc_gu[...] = jnp.zeros_like(acc_gu)
    acc_d[...] = jnp.zeros_like(acc_d)
    acc_b[...] = jnp.zeros_like(acc_b)
    for c in loads:
        c.wait()

    def step(k, carry):
        for j, places in ARRIVALS.items():
            @pl.when(k == j)
            def _():
                for place in places:
                    arrive(SLOT[place])
        remote(x_own.at[k], x_sib.at[k], ag_send.at[0], sib_recv.at[k, 0], sib).wait_recv()
        remote(g_own.at[k], g_sib.at[k], ag_send.at[0], sib_recv.at[k, 1], sib).wait_recv()
        compute(k)
        for c in to_sibling(k):
            c.start()

        @pl.when(k >= LAG)
        def _():
            add_sibling(k - LAG)
        for j, df in FIRST_AT.items():
            @pl.when(k == j)
            def _():
                for c in s_first(df):
                    c.start()
        for j, df in SECOND_AT.items():
            @pl.when(k == j)
            def _():
                send_second(df)
        return carry

    lax.fori_loop(0, N_SLOT, step, 0)

    stores = []
    for e in range(n_loc):
        cols = pl.ds(e * width, width)
        stores.append(pltpu.make_async_copy(acc_gu.at[:, cols], dwg_ref.at[e], load_sem.at[len(stores)]))
        stores.append(pltpu.make_async_copy(acc_gu.at[:, pl.ds(loc + e * width, width)], dwu_ref.at[e], load_sem.at[len(stores)]))
        stores.append(pltpu.make_async_copy(acc_d.at[cols], dwd_ref.at[e], load_sem.at[len(stores)]))
    for c in stores:
        c.start()
    dbias_ref[...] = jnp.sum(acc_b[...], axis=0, keepdims=True)
    for j in range(N_SLOT - LAG, N_SLOT):
        add_sibling(j)
    send_second(2)

    k2, k1, k3 = SLOT[(2, 0)], SLOT[(1, 0)], SLOT[(3, 0)]

    def wait_second(df):
        for i in range(2):
            for c in s_second(df, i):
                c.wait_recv()
        pg_own[SLOT[(df, 0)]] = pg_own[SLOT[(df, 0)]] + r2g[df, 0] + r2g[df, 1]

    def total(k, df, t):
        return part[k, t].astype(F32) + r2[df, 0, t].astype(F32) + r2[df, 1, t].astype(F32)

    f_first = (remote(pg_own.at[k2], r3g, f1_send.at[2], f1_recv.at[2], f_up),
               remote(part.at[k2, 0], r3.at[0], f1_send.at[0], f1_recv.at[0], f_up),
               remote(part.at[k2, 1], r3.at[1], f1_send.at[1], f1_recv.at[1], f_dn))
    f_second = (remote(pg_own.at[k1], r4g.at[0], f2_send.at[1], f2_recv.at[1], f_up),
                remote(pg_own.at[k3], r4g.at[1], f2_send.at[3], f2_recv.at[3], f_dn),
                remote(part.at[k1], r4.at[0], f2_send.at[0], f2_recv.at[0], f_up),
                remote(part.at[k3], r4.at[1], f2_send.at[2], f2_recv.at[2], f_dn))
    for df, k in ((1, k1), (3, k3), (0, 0), (2, k2)):
        wait_second(df)
        if df:
            part[k, 0] = total(k, df, 0).astype(BF16)
            part[k, 1] = total(k, df, 1).astype(BF16)
    for c in f_first:
        c.start()
    for c in f_first:
        c.wait_recv()
    pg_own[k1] = pg_own[k1] + r3g[...]
    add_into(k1, 0, r3.at[0])
    add_into(k3, 1, r3.at[1])
    for c in f_second:
        c.start()

    for c in f_second[:2]:
        c.wait_recv()
    gates = g_own[0]
    d_gates = jnp.where(chosen_mask(), pg_own[0] + r4g[0] + r4g[1], 0.0)
    d_logits = gates * (d_gates - jnp.sum(gates * d_gates, axis=0, keepdims=True))
    dl_buf[0, 0] = d_logits
    dh_router = lax.dot_general(d_logits, router_ref[...].astype(F32), (((0,), (0,)), ((), ())), precision=lax.Precision.HIGHEST, preferred_element_type=F32)
    f_dl = [remote(dl_buf.at[0, 0], dl_buf.at[0, to], e_send.at[i], e_recv.at[i], dev) for i, (to, dev) in enumerate(((3, f_up), (1, f_dn), (2, f_op)))]
    s_dl = [remote(dl_buf.at[0], dl_buf.at[to], e_send.at[3 + i], e_recv.at[3 + i], dev) for i, (to, dev) in enumerate(((3, s_up), (1, s_dn), (2, s_op)))]
    for c in f_dl:
        c.start()
    for c in f_dl:
        c.wait_recv()
    for c in s_dl:
        c.start()
    for c in s_dl:
        c.wait_recv()
    d_router = jnp.zeros((n_exp, d_model), F32)
    for k, (df, ds) in enumerate(ORDER):
        dl = dl_buf[ds, df]
        dl_hi = dl.astype(BF16)
        dl_lo = (dl - dl_hi.astype(F32)).astype(BF16)
        prods = jnp.dot(jnp.concatenate([dl_hi, dl_lo], axis=0), x_own[k, 0], preferred_element_type=F32)
        d_router = d_router + (prods[:n_exp] + prods[n_exp:])
    dr_buf[0] = d_router

    for c in f_second[2:]:
        c.wait_recv()
    sib_dr = remote(dr_buf.at[0], dr_buf.at[1], e_send.at[6], e_recv.at[6], sib)
    sib_dr.start()
    x, inv_rms, normed = normalised()
    dh_total = total(0, 0, 1) + r4[0, 1].astype(F32) + r4[1, 1].astype(F32) + dh_router
    gn_buf[0] = jnp.sum(dh_total * normed, axis=0, keepdims=True)
    d_norm = dh_total * gain
    dx_ref[...] = (dy_ref[...].astype(F32) + inv_rms * (d_norm - normed * jnp.mean(d_norm * normed, axis=-1, keepdims=True))).astype(BF16)
    exchanges = [sib_dr]
    n_sem = 7
    for group in ((f_up, f_dn, f_op), (s_up, s_dn, s_op), (sib,)):
        base = n_sem - 7
        copies = [remote(gn_buf.at[base], gn_buf.at[base + 1 + i], e_send.at[n_sem + i], e_recv.at[n_sem + i], dev) for i, dev in enumerate(group)]
        for c in copies:
            c.start()
        if base == 0:
            y_moe = total(0, 0, 0) + r4[0, 0].astype(F32) + r4[1, 0].astype(F32)
            y_ref[...] = (x + (y_moe + bias_ref[...].astype(F32))).astype(BF16)
        for c in copies:
            c.wait_recv()
        summed = gn_buf[base]
        for i in range(len(group)):
            summed = summed + gn_buf[base + 1 + i]
        exchanges += copies
        n_sem += len(group) + 1
        if len(group) > 1:
            gn_buf[n_sem - 7] = summed
        else:
            dgain_ref[...] = summed
    sib_dr.wait_recv()
    drouter_ref[...] = dr_buf[0] + dr_buf[1]

    for c in f_dl + s_dl + exchanges:
        c.wait_send()
    for c in stores:
        c.wait()
    for k in range(N_SLOT):
        for make in sends[k]:
            make().wait_send()
        for c in to_sibling(k):
            c.wait_send()
    for df in range(4):
        for c in s_first(df):
            c.wait_send()
        for i in range(2):
            for c in s_second(df, i):
                c.wait_send()
    for c in f_first + f_second:
        c.wait_send()


def moe(x, dy, idx_t, gain, bias, router_t, w_gate, w_up, w_down):
    n_tok, d_model = x.shape
    n_loc, _, width = w_gate.shape
    n_exp = router_t.shape[0]
    loc = n_loc * width
    vmem = pl.BlockSpec(memory_space=pltpu.VMEM)
    hbm = pl.BlockSpec(memory_space=pl.ANY)
    block = (2, n_tok, d_model)
    small = (n_exp, n_tok)
    dma = pltpu.SemaphoreType.DMA
    scratch = [
        pltpu.VMEM((N_SLOT, *block), BF16), pltpu.VMEM((N_SLOT, *block), BF16), pltpu.VMEM((N_SLOT, *block), BF16),
        pltpu.VMEM((N_SLOT, *small), F32), pltpu.VMEM((N_SLOT, *small), F32),
        pltpu.VMEM((N_SLOT, *small), F32), pltpu.VMEM((N_SLOT, *small), F32),
        pltpu.VMEM((N_SLOT, *block), BF16), pltpu.VMEM((N_SLOT, *small), F32),
        pltpu.VMEM((4, *block), BF16), pltpu.VMEM((4, *small), F32),
        pltpu.VMEM((4, 2, *block), BF16), pltpu.VMEM((4, 2, *small), F32),
        pltpu.VMEM(block, BF16), pltpu.VMEM(small, F32),
        pltpu.VMEM((2, *block), BF16), pltpu.VMEM((2, *small), F32),
        pltpu.VMEM((4, 4, *small), F32), pltpu.VMEM((2, n_exp, d_model), F32), pltpu.VMEM((10, 1, d_model), F32),
        pltpu.VMEM((d_model, 2 * loc), BF16), pltpu.VMEM((loc, d_model), BF16),
        pltpu.VMEM((d_model, 2 * loc), F32), pltpu.VMEM((loc, d_model), F32), pltpu.VMEM((8, d_model), F32),
        dma((3 * n_loc,)), dma((N_SEND,)), dma((N_SLOT, 2)), dma((N_SLOT,)), dma((N_SLOT, 2)),
        dma((N_SLOT, 2)), dma((N_SLOT, 2)), dma((4, 3)), dma((4, 3)), dma((4, 2, 2)), dma((4, 2, 2)),
        dma((3,)), dma((3,)), dma((4,)), dma((4,)), dma((17,)), dma((17,)),
    ]
    out_shape = (
        jax.ShapeDtypeStruct((n_tok, d_model), BF16), jax.ShapeDtypeStruct((n_tok, d_model), BF16),
        jax.ShapeDtypeStruct((1, d_model), F32), jax.ShapeDtypeStruct((n_exp, d_model), F32), jax.ShapeDtypeStruct((1, d_model), F32),
        jax.ShapeDtypeStruct(w_gate.shape, F32), jax.ShapeDtypeStruct(w_up.shape, F32), jax.ShapeDtypeStruct(w_down.shape, F32),
    )
    return pl.pallas_call(
        moe_kernel, name="moe", out_shape=out_shape,
        in_specs=[vmem] * 6 + [hbm] * 3, out_specs=(vmem,) * 5 + (hbm,) * 3,
        scratch_shapes=scratch,
        compiler_params=pltpu.CompilerParams(collective_id=0, has_side_effects=True, vmem_limit_bytes=67_043_328),
    )(x, dy, idx_t, gain, bias, router_t, w_gate, w_up, w_down)


def solution(mesh):
    tok_spec = P(("dp", "ep", "tp"), None)
    wide_spec = P("ep", None, "tp")
    down_spec = P("ep", "tp", None)
    grad_wide = P(("dp", "ep"), None, "tp")
    grad_down = P(("dp", "ep"), "tp", None)

    def device_step(x_in, norm_gain, w_router, expert_idx, w_gate, w_up, w_down, out_bias, dy_out):
        y_out, dx_in, d_gain, d_router_t, d_bias, d_gate, d_up, d_down = moe(
            x_in, dy_out, expert_idx.T, norm_gain[None, :], out_bias[None, :], w_router.T, w_gate, w_up, w_down)
        return y_out, dx_in, d_gain[0], d_router_t.T, d_gate, d_up, d_down, d_bias[0]

    return jax.shard_map(device_step, mesh=mesh, in_specs=(tok_spec, P(None), P(None, None), tok_spec, wide_spec, wide_spec, down_spec, P(None), tok_spec), out_specs=(tok_spec, tok_spec, P("dp"), P("dp", None), grad_wide, grad_wide, grad_down, P("dp")), check_vma=False)
```

```python
import jax
import jax.numpy as jnp
from jax import lax
from jax.experimental import pallas as pl
from jax.experimental.pallas import tpu as pltpu
from jax.sharding import PartitionSpec as P

EPS = 1e-6
MESH = pl.DeviceIdType.MESH
F32 = jnp.float32
BF16 = jnp.bfloat16
ORDER = ((0, 0), (0, 1), (0, 3), (0, 2), (1, 0), (1, 1), (1, 3), (2, 1), (2, 3), (3, 1), (1, 2), (2, 2), (3, 3), (3, 2), (2, 0), (3, 0))
ARRIVALS = {1: ((0, 1), (0, 3), (1, 0), (3, 0)), 2: ((2, 0), (0, 2)), 4: ((1, 1), (1, 3)), 6: ((2, 1), (2, 3)),
            8: ((3, 1), (3, 3)), 9: ((1, 2),), 10: ((2, 2),), 11: ((3, 2),)}
FIRST_AT = {8: 0, 11: 1, 12: 2, 14: 3}
SECOND_AT = {10: 0, 13: 1, 14: 2}
SLOT = {place: k for k, place in enumerate(ORDER)}
N_SLOT = len(ORDER)
N_SEND = 67
LAG = 1


def dot_nt(a, b):
    return lax.dot_general(a, b, (((1,), (1,)), ((), ())), preferred_element_type=F32)


def moe_kernel(x_ref, dy_ref, idx_ref, gain_ref, bias_ref, router_ref, wg_ref, wu_ref, wd_ref,
               y_ref, dx_ref, dgain_ref, drouter_ref, dbias_ref, dwg_ref, dwu_ref, dwd_ref,
               x_own, x_sib, part, g_own, g_sib, pg_own, pg_sib, q_buf, qg_buf,
               r1, r1g, r2, r2g, r3, r3g, r4, r4g, dl_buf, dr_buf, gn_buf, wgu, wd, acc_gu, acc_d, acc_b,
               load_sem, ag_send, ag_recv, ag_grecv, sib_recv,
               rq_send, rq_recv, s1_send, s1_recv, s2_send, s2_recv, f1_send, f1_recv, f2_send, f2_recv, e_send, e_recv):
    ep = lax.axis_index("ep")
    tp = lax.axis_index("tp")
    n_tp = lax.axis_size("tp")
    n_x = lax.axis_size("ep") // 2
    core = lax.rem(ep, 2)
    chip_x = lax.div(ep, 2)
    n_loc, d_model, width = wg_ref.shape
    n_tok = x_ref.shape[0]
    n_exp = router_ref.shape[0]
    loc = n_loc * width

    def shifted(x_step, y_step):
        x_new = lax.rem(chip_x + x_step + n_x, n_x)
        y_new = lax.rem(tp + y_step + n_tp, n_tp)
        return {"tp": y_new, "ep": 2 * x_new + core}

    f_up = shifted(1 - core, core)
    f_dn = shifted(core - 1, -core)
    s_up = shifted(core, 1 - core)
    s_dn = shifted(-core, core - 1)
    f_op = shifted(2 * (1 - core), 2 * core)
    s_op = shifted(2 * core, 2 * (1 - core))
    sib = {"ep": ep + 1 - 2 * core}

    loads = []
    for e in range(n_loc):
        cols = pl.ds(e * width, width)
        loads.append(pltpu.make_async_copy(wg_ref.at[e], wgu.at[:, cols], load_sem.at[len(loads)]))
        loads.append(pltpu.make_async_copy(wu_ref.at[e], wgu.at[:, pl.ds(loc + e * width, width)], load_sem.at[len(loads)]))
        loads.append(pltpu.make_async_copy(wd_ref.at[e], wd.at[cols], load_sem.at[len(loads)]))
    for c in loads:
        c.start()
    barrier = pltpu.get_barrier_semaphore()
    peers = (f_up, f_dn, f_op, s_up, s_dn, s_op, sib)
    for dev in peers:
        pl.semaphore_signal(barrier, inc=1, device_id=dev, device_id_type=MESH)

    def normalised():
        x = x_ref[...].astype(F32)
        inv_rms = lax.rsqrt(jnp.mean(x * x, axis=-1, keepdims=True) + EPS)
        return x, inv_rms, x * inv_rms

    def chosen_mask():
        expert = lax.broadcasted_iota(jnp.int32, (n_exp, n_tok), 0)
        chosen = expert == idx_ref[0:1, :]
        for j in range(1, idx_ref.shape[0]):
            chosen = jnp.logical_or(chosen, expert == idx_ref[j:j + 1, :])
        return chosen

    gain = gain_ref[...].astype(F32).reshape(1, d_model)
    hidden = (normalised()[2] * gain).astype(BF16)
    x_own[0, 0] = hidden
    x_own[0, 1] = dy_ref[...]
    logits = jnp.where(chosen_mask(), dot_nt(router_ref[...], hidden), -jnp.inf)
    weight = jnp.exp(logits - jnp.max(logits, axis=0, keepdims=True))
    g_own[0] = weight / jnp.sum(weight, axis=0, keepdims=True)
    pl.semaphore_wait(barrier, len(peers))

    def remote(src, dst, send, recv, dev):
        return pltpu.make_async_remote_copy(src_ref=src, dst_ref=dst, send_sem=send, recv_sem=recv, device_id=dev, device_id_type=MESH)

    sends = {k: [] for k in (*range(N_SLOT), "late")}
    count = [0]

    def plan(k, src, dst, recv, dev):
        n = count[0]
        count[0] += 1
        sends[k].append(lambda: remote(src, dst, ag_send.at[n], recv, dev))

    def plan_block(k, to, dev, after=None):
        after = k if after is None else after
        plan(after, x_own.at[k], x_own.at[to], ag_recv.at[to, 0], dev)
        plan(after, g_own.at[k], g_own.at[to], ag_grecv.at[to], dev)

    plan_block(0, SLOT[(3, 0)], f_up)
    plan_block(0, SLOT[(1, 0)], f_dn)
    for k, (df, ds) in enumerate(ORDER):
        if (df, ds) == (3, 0):
            to = SLOT[(2, 0)]
            plan(k, x_own.at[k, 0], x_own.at[to, 0], ag_recv.at[to, 0], f_up)
            plan(k, g_own.at[k], g_own.at[to], ag_grecv.at[to], f_up)
        if (df, ds) == (1, 0):
            to = SLOT[(2, 0)]
            plan(k, x_own.at[k, 1], x_own.at[to, 1], ag_recv.at[to, 1], f_dn)
        if ds == 0:
            after = "late" if (df, ds) == (3, 0) else k
            plan_block(k, SLOT[(df, 3)], s_up, after)
            plan_block(k, SLOT[(df, 1)], s_dn, after)
        if ds == 3:
            to = SLOT[(df, 2)]
            plan(k, x_own.at[k, 0], x_own.at[to, 0], ag_recv.at[to, 0], s_up)
            plan(k, g_own.at[k], g_own.at[to], ag_grecv.at[to], s_up)
        if ds == 1:
            to = SLOT[(df, 2)]
            plan(k, x_own.at[k, 1], x_own.at[to, 1], ag_recv.at[to, 1], s_dn)
        plan(k, x_own.at[k], x_sib.at[k], sib_recv.at[k, 0], sib)
        plan(k, g_own.at[k], g_sib.at[k], sib_recv.at[k, 1], sib)
    assert count[0] == N_SEND

    def arrive(k):
        if k:
            if ORDER[k][1] == 2 or ORDER[k] == (2, 0):
                for t in range(2):
                    remote(x_own.at[k, t], x_own.at[k, t], ag_send.at[0], ag_recv.at[k, t], sib).wait_recv()
            else:
                remote(x_own.at[k], x_own.at[k], ag_send.at[0], ag_recv.at[k, 0], sib).wait_recv()
            remote(g_own.at[k], g_own.at[k], ag_send.at[0], ag_grecv.at[k], sib).wait_recv()
        for make in sends[k] + (sends["late"] if ORDER[k] == (2, 0) else []):
            make().start()

    def to_sibling(k):
        return (remote(x_sib.at[k], q_buf.at[k], rq_send.at[k, 0], rq_recv.at[k, 0], sib),
                remote(pg_sib.at[k], qg_buf.at[k], rq_send.at[k, 1], rq_recv.at[k, 1], sib))

    def add_sibling(k):
        for c in to_sibling(k):
            c.wait_recv()
        part[k] = (part[k].astype(F32) + q_buf[k].astype(F32)).astype(BF16)
        pg_own[k] = pg_own[k] + qg_buf[k]

    def s_first(df):
        k = SLOT[(df, 2)]
        return (remote(part.at[k, 0], r1.at[df, 0], s1_send.at[df, 0], s1_recv.at[df, 0], s_up),
                remote(part.at[k, 1], r1.at[df, 1], s1_send.at[df, 1], s1_recv.at[df, 1], s_dn),
                remote(pg_own.at[k], r1g.at[df], s1_send.at[df, 2], s1_recv.at[df, 2], s_up))

    def s_second(df, i):
        k = SLOT[(df, (1, 3)[i])]
        dev = (s_up, s_dn)[i]
        return (remote(pg_own.at[k], r2g.at[df, i], s2_send.at[df, i, 1], s2_recv.at[df, i, 1], dev),
                remote(part.at[k], r2.at[df, i], s2_send.at[df, i, 0], s2_recv.at[df, i, 0], dev))

    def add_into(k, t, block):
        part[k, t] = (part[k, t].astype(F32) + block[...].astype(F32)).astype(BF16)

    def send_second(df):
        for c in s_first(df):
            c.wait_recv()
        k = SLOT[(df, 1)]
        add_into(k, 0, r1.at[df, 0])
        pg_own[k] = pg_own[k] + r1g[df]
        add_into(SLOT[(df, 3)], 1, r1.at[df, 1])
        for i in range(2):
            for c in s_second(df, i):
                c.start()

    row = lax.broadcasted_iota(jnp.int32, (n_exp, loc), 0)
    col = lax.broadcasted_iota(jnp.int32, (n_exp, loc), 1)
    pick = jnp.where(row == ep * n_loc + lax.div(col, width), 1.0, 0.0).astype(F32)

    def widen(g):
        return lax.dot_general(g, pick, (((0,), (0,)), ((), ())), precision=lax.Precision.HIGHEST, preferred_element_type=F32)

    def compute(k):
        h = jnp.concatenate([x_own[k, 0], x_sib[k, 0]], axis=0)
        dy = jnp.concatenate([x_own[k, 1], x_sib[k, 1]], axis=0)
        gate = jnp.concatenate([widen(g_own[k]), widen(g_sib[k])], axis=0)
        both = jnp.dot(h, wgu[...], preferred_element_type=F32)
        g_pre = both[:, :loc]
        u_pre = both[:, loc:]
        d_raw = dot_nt(dy, wd[...])
        used = gate != 0.0
        sig = jax.nn.sigmoid(g_pre)
        silu = g_pre * sig
        act = (silu * u_pre).astype(BF16).astype(F32)
        act_g = jnp.where(used, gate * act, 0.0).astype(BF16)
        prod = jnp.where(used, act * d_raw, 0.0)
        d_act = gate * d_raw
        d_g = jnp.where(used, d_act * u_pre * sig * (1.0 + g_pre * (1.0 - sig)), 0.0).astype(BF16)
        d_u = jnp.where(used, d_act * silu, 0.0).astype(BF16)
        d_gu = jnp.concatenate([d_g, d_u], axis=1)
        prod_hi = prod.astype(BF16)
        prod_lo = (prod - prod_hi.astype(F32)).astype(BF16)
        pick_b = pick.astype(BF16)
        dgate = dot_nt(pick_b, prod_hi) + dot_nt(pick_b, prod_lo)
        pg_own[k] = dgate[:, :n_tok]
        pg_sib[k] = dgate[:, n_tok:]
        acc_b[...] += jnp.sum(dy.astype(F32).reshape(2 * n_tok // 8, 8, d_model), axis=0)
        acc_gu[...] += jnp.dot(h.T, d_gu, preferred_element_type=F32)
        acc_d[...] += jnp.dot(act_g.T, dy, preferred_element_type=F32)
        y = jnp.dot(act_g, wd[...], preferred_element_type=F32).astype(BF16)
        part[k, 0] = y[:n_tok]
        x_sib[k, 0] = y[n_tok:]
        dh = dot_nt(d_gu, wgu[...]).astype(BF16)
        part[k, 1] = dh[:n_tok]
        x_sib[k, 1] = dh[n_tok:]

    arrive(0)
    acc_gu[...] = jnp.zeros_like(acc_gu)
    acc_d[...] = jnp.zeros_like(acc_d)
    acc_b[...] = jnp.zeros_like(acc_b)
    for c in loads:
        c.wait()

    def step(k, carry):
        for j, places in ARRIVALS.items():
            @pl.when(k == j)
            def _():
                for place in places:
                    arrive(SLOT[place])
        remote(x_own.at[k], x_sib.at[k], ag_send.at[0], sib_recv.at[k, 0], sib).wait_recv()
        remote(g_own.at[k], g_sib.at[k], ag_send.at[0], sib_recv.at[k, 1], sib).wait_recv()
        compute(k)
        for c in to_sibling(k):
            c.start()

        @pl.when(k >= LAG)
        def _():
            add_sibling(k - LAG)
        for j, df in FIRST_AT.items():
            @pl.when(k == j)
            def _():
                for c in s_first(df):
                    c.start()
        for j, df in SECOND_AT.items():
            @pl.when(k == j)
            def _():
                send_second(df)
        return carry

    lax.fori_loop(0, N_SLOT, step, 0)

    stores = []
    for e in range(n_loc):
        cols = pl.ds(e * width, width)
        stores.append(pltpu.make_async_copy(acc_gu.at[:, cols], dwg_ref.at[e], load_sem.at[len(stores)]))
        stores.append(pltpu.make_async_copy(acc_gu.at[:, pl.ds(loc + e * width, width)], dwu_ref.at[e], load_sem.at[len(stores)]))
        stores.append(pltpu.make_async_copy(acc_d.at[cols], dwd_ref.at[e], load_sem.at[len(stores)]))
    for c in stores:
        c.start()
    dbias_ref[...] = jnp.sum(acc_b[...], axis=0, keepdims=True)
    for j in range(N_SLOT - LAG, N_SLOT):
        add_sibling(j)
    send_second(3)

    k2, k1, k3 = SLOT[(2, 0)], SLOT[(1, 0)], SLOT[(3, 0)]

    def wait_second(df):
        for i in range(2):
            for c in s_second(df, i):
                c.wait_recv()
        pg_own[SLOT[(df, 0)]] = pg_own[SLOT[(df, 0)]] + r2g[df, 0] + r2g[df, 1]

    def total(k, df, t):
        return part[k, t].astype(F32) + r2[df, 0, t].astype(F32) + r2[df, 1, t].astype(F32)

    f_first = (remote(pg_own.at[k2], r3g, f1_send.at[2], f1_recv.at[2], f_up),
               remote(part.at[k2, 0], r3.at[0], f1_send.at[0], f1_recv.at[0], f_up),
               remote(part.at[k2, 1], r3.at[1], f1_send.at[1], f1_recv.at[1], f_dn))
    f_second = (remote(pg_own.at[k1], r4g.at[0], f2_send.at[0], f2_recv.at[0], f_up),
                remote(pg_own.at[k3], r4g.at[1], f2_send.at[1], f2_recv.at[1], f_dn),
                remote(part.at[k1, 1], r4.at[0, 1], f2_send.at[2], f2_recv.at[2], f_up),
                remote(part.at[k3, 1], r4.at[1, 1], f2_send.at[3], f2_recv.at[3], f_dn),
                remote(part.at[k1, 0], r4.at[0, 0], f2_send.at[4], f2_recv.at[4], f_up),
                remote(part.at[k3, 0], r4.at[1, 0], f2_send.at[5], f2_recv.at[5], f_dn))
    for df, k in ((2, k2), (1, k1), (3, k3)):
        wait_second(df)
        part[k, 0] = total(k, df, 0).astype(BF16)
        part[k, 1] = total(k, df, 1).astype(BF16)
        if df == 2:
            for c in f_first:
                c.start()
        if df == 1:
            f_first[0].wait_recv()
            pg_own[k1] = pg_own[k1] + r3g[...]
            f_second[0].start()
            f_second[2].start()
            f_first[1].wait_recv()
            add_into(k1, 0, r3.at[0])
            f_second[4].start()
    f_second[1].start()
    f_first[2].wait_recv()
    add_into(k3, 1, r3.at[1])
    f_second[3].start()
    f_second[5].start()
    wait_second(0)

    for c in f_second[:2]:
        c.wait_recv()
    gates = g_own[0]
    d_gates = jnp.where(chosen_mask(), pg_own[0] + r4g[0] + r4g[1], 0.0)
    d_logits = gates * (d_gates - jnp.sum(gates * d_gates, axis=0, keepdims=True))
    dl_buf[0, 0] = d_logits
    dh_router = lax.dot_general(d_logits, router_ref[...].astype(F32), (((0,), (0,)), ((), ())), precision=lax.Precision.HIGHEST, preferred_element_type=F32)
    s_dl = [remote(dl_buf.at[0, 0], dl_buf.at[0, to], e_send.at[i], e_recv.at[i], dev) for i, (to, dev) in enumerate(((3, s_up), (1, s_dn), (2, s_op)))]
    f_dl = [remote(dl_buf.at[0], dl_buf.at[to], e_send.at[3 + i], e_recv.at[3 + i], dev) for i, (to, dev) in enumerate(((3, f_up), (1, f_dn), (2, f_op)))]
    for c in s_dl:
        c.start()

    for c in f_second[2:4]:
        c.wait_recv()
    x, inv_rms, normed = normalised()
    dh_total = total(0, 0, 1) + r4[0, 1].astype(F32) + r4[1, 1].astype(F32) + dh_router
    gn_buf[0] = jnp.sum(dh_total * normed, axis=0, keepdims=True)

    def exchange(base, group, first_sem):
        return [remote(gn_buf.at[base], gn_buf.at[base + 1 + i], e_send.at[first_sem + i], e_recv.at[first_sem + i], dev) for i, dev in enumerate(group)]

    def gathered(base, copies):
        for c in copies:
            c.wait_recv()
        summed = gn_buf[base]
        for i in range(len(copies)):
            summed = summed + gn_buf[base + 1 + i]
        return summed

    gn_sib = exchange(0, (sib,), 7)
    for c in gn_sib:
        c.start()
    for c in s_dl:
        c.wait_recv()
    for c in f_dl:
        c.start()
    d_norm = dh_total * gain
    dx_ref[...] = (dy_ref[...].astype(F32) + inv_rms * (d_norm - normed * jnp.mean(d_norm * normed, axis=-1, keepdims=True))).astype(BF16)
    gn_buf[2] = gathered(0, gn_sib)
    gn_s = exchange(2, (s_up, s_dn, s_op), 8)
    for c in gn_s:
        c.start()
    d_router = jnp.zeros((n_exp, d_model), F32)
    for c in f_dl:
        c.wait_recv()
    for k, (df, ds) in enumerate(ORDER):
        dl = dl_buf[df, ds]
        dl_hi = dl.astype(BF16)
        dl_lo = (dl - dl_hi.astype(F32)).astype(BF16)
        prods = jnp.dot(jnp.concatenate([dl_hi, dl_lo], axis=0), x_own[k, 0], preferred_element_type=F32)
        d_router = d_router + (prods[:n_exp] + prods[n_exp:])
        if k == 3:
            gn_buf[6] = gathered(2, gn_s)
            gn_f = exchange(6, (f_up, f_dn, f_op), 11)
            for c in gn_f:
                c.start()
    dr_buf[0] = d_router
    sib_dr = remote(dr_buf.at[0], dr_buf.at[1], e_send.at[6], e_recv.at[6], sib)
    sib_dr.start()
    for c in f_second[4:]:
        c.wait_recv()
    y_moe = total(0, 0, 0) + r4[0, 0].astype(F32) + r4[1, 0].astype(F32)
    y_ref[...] = (x + (y_moe + bias_ref[...].astype(F32).reshape(1, d_model))).astype(BF16)
    dgain_ref[...] = gathered(6, gn_f)
    sib_dr.wait_recv()
    drouter_ref[...] = dr_buf[0] + dr_buf[1]

    for c in f_dl + s_dl + gn_sib + gn_s + gn_f + [sib_dr]:
        c.wait_send()
    for c in stores:
        c.wait()
    for made in sends.values():
        for make in made:
            make().wait_send()
    for k in range(N_SLOT):
        for c in to_sibling(k):
            c.wait_send()
    for df in range(4):
        for c in s_first(df):
            c.wait_send()
        for i in range(2):
            for c in s_second(df, i):
                c.wait_send()
    for c in f_first + f_second:
        c.wait_send()


def moe(x, dy, idx_t, gain, bias, router_t, w_gate, w_up, w_down):
    n_tok, d_model = x.shape
    n_loc, _, width = w_gate.shape
    n_exp = router_t.shape[0]
    loc = n_loc * width
    vmem = pl.BlockSpec(memory_space=pltpu.VMEM)
    hbm = pl.BlockSpec(memory_space=pl.ANY)
    block = (2, n_tok, d_model)
    small = (n_exp, n_tok)
    dma = pltpu.SemaphoreType.DMA
    scratch = [
        pltpu.VMEM((N_SLOT, *block), BF16), pltpu.VMEM((N_SLOT, *block), BF16), pltpu.VMEM((N_SLOT, *block), BF16),
        pltpu.VMEM((N_SLOT, *small), F32), pltpu.VMEM((N_SLOT, *small), F32),
        pltpu.VMEM((N_SLOT, *small), F32), pltpu.VMEM((N_SLOT, *small), F32),
        pltpu.VMEM((N_SLOT, *block), BF16), pltpu.VMEM((N_SLOT, *small), F32),
        pltpu.VMEM((4, *block), BF16), pltpu.VMEM((4, *small), F32),
        pltpu.VMEM((4, 2, *block), BF16), pltpu.VMEM((4, 2, *small), F32),
        pltpu.VMEM(block, BF16), pltpu.VMEM(small, F32),
        pltpu.VMEM((2, *block), BF16), pltpu.VMEM((2, *small), F32),
        pltpu.VMEM((4, 4, *small), F32), pltpu.VMEM((2, n_exp, d_model), F32), pltpu.VMEM((10, 1, d_model), F32),
        pltpu.VMEM((d_model, 2 * loc), BF16), pltpu.VMEM((loc, d_model), BF16),
        pltpu.VMEM((d_model, 2 * loc), F32), pltpu.VMEM((loc, d_model), F32), pltpu.VMEM((8, d_model), F32),
        dma((3 * n_loc,)), dma((N_SEND,)), dma((N_SLOT, 2)), dma((N_SLOT,)), dma((N_SLOT, 2)),
        dma((N_SLOT, 2)), dma((N_SLOT, 2)), dma((4, 3)), dma((4, 3)), dma((4, 2, 2)), dma((4, 2, 2)),
        dma((3,)), dma((3,)), dma((6,)), dma((6,)), dma((14,)), dma((14,)),
    ]
    out_shape = (
        jax.ShapeDtypeStruct((n_tok, d_model), BF16), jax.ShapeDtypeStruct((n_tok, d_model), BF16),
        jax.ShapeDtypeStruct((1, d_model), F32), jax.ShapeDtypeStruct((n_exp, d_model), F32), jax.ShapeDtypeStruct((1, d_model), F32),
        jax.ShapeDtypeStruct(w_gate.shape, F32), jax.ShapeDtypeStruct(w_up.shape, F32), jax.ShapeDtypeStruct(w_down.shape, F32),
    )
    return pl.pallas_call(
        moe_kernel, name="moe", out_shape=out_shape,
        in_specs=[vmem] * 6 + [hbm] * 3, out_specs=(vmem,) * 5 + (hbm,) * 3,
        scratch_shapes=scratch,
        compiler_params=pltpu.CompilerParams(collective_id=0, has_side_effects=True, vmem_limit_bytes=67_043_328),
    )(x, dy, idx_t, gain, bias, router_t, w_gate, w_up, w_down)


def write_out(*refs):
    n = len(refs) // 3
    sources, results, rooms, sems = refs[:n], refs[n:2 * n], refs[2 * n:3 * n], refs[3 * n]
    pieces = []
    for i in range(n):
        for j in range(sources[i].shape[0] if len(sources[i].shape) == 3 else 1):
            at = (lambda r, j=j: r.at[j]) if len(sources[i].shape) == 3 else (lambda r: r)
            m = len(pieces)
            pieces.append((pltpu.make_async_copy(at(sources[i]), at(rooms[i]), sems.at[m, 0]),
                           pltpu.make_async_copy(at(rooms[i]), at(results[i]), sems.at[m, 1])))
    for load, _ in pieces:
        load.start()
    for load, store in pieces:
        load.wait()
        store.start()
    for _, store in pieces:
        store.wait()


def finish(*arrays):
    hbm = pl.BlockSpec(memory_space=pl.ANY)
    n_pieces = sum(a.shape[0] if a.ndim == 3 else 1 for a in arrays)
    return pl.pallas_call(
        write_out, name="finish", out_shape=tuple(jax.ShapeDtypeStruct(a.shape, a.dtype) for a in arrays),
        in_specs=[hbm] * len(arrays), out_specs=(hbm,) * len(arrays),
        scratch_shapes=[pltpu.VMEM(a.shape, a.dtype) for a in arrays] + [pltpu.SemaphoreType.DMA((n_pieces, 2))],
        compiler_params=pltpu.CompilerParams(vmem_limit_bytes=32 << 20),
    )(*arrays)


def solution(mesh):
    tok_spec = P(("dp", "ep", "tp"), None)
    wide_spec = P("ep", None, "tp")
    down_spec = P("ep", "tp", None)
    grad_wide = P(("dp", "ep"), None, "tp")
    grad_down = P(("dp", "ep"), "tp", None)

    def device_step(x_in, norm_gain, w_router, expert_idx, w_gate, w_up, w_down, out_bias, dy_out):
        y_out, dx_in, d_gain, d_router_t, d_bias, d_gate, d_up, d_down = moe(
            x_in, dy_out, expert_idx.T, norm_gain, out_bias, w_router.T, w_gate, w_up, w_down)
        y_out, dx_in, d_gate, d_up, d_down = finish(y_out, dx_in, d_gate, d_up, d_down)
        return y_out, dx_in, d_gain[0], d_router_t.T, d_gate, d_up, d_down, d_bias[0]

    return jax.shard_map(device_step, mesh=mesh, in_specs=(tok_spec, P(None), P(None, None), tok_spec, wide_spec, wide_spec, down_spec, P(None), tok_spec), out_specs=(tok_spec, tok_spec, P("dp"), P("dp", None), grad_wide, grad_wide, grad_down, P("dp")), check_vma=False)
```

```python
import jax
import jax.numpy as jnp
from jax import lax
from jax.experimental import pallas as pl
from jax.experimental.pallas import tpu as pltpu
from jax.sharding import PartitionSpec as P

EPS = 1e-6
MESH = pl.DeviceIdType.MESH
F32 = jnp.float32
BF16 = jnp.bfloat16
ORDER = ((0, 0), (0, 1), (0, 3), (0, 2), (1, 0), (1, 1), (1, 3), (2, 1), (2, 3), (3, 1), (1, 2), (2, 2), (3, 3), (3, 2), (2, 0), (3, 0))
ARRIVALS = {1: ((0, 1), (0, 3)), 2: ((1, 0), (3, 0), (0, 2)), 3: ((2, 0),), 4: ((1, 1), (1, 3)), 6: ((2, 1), (2, 3)),
            8: ((3, 1), (3, 3)), 9: ((1, 2),), 10: ((2, 2),), 11: ((3, 2),)}
FIRST_AT = {8: 0, 11: 1, 12: 2, 14: 3}
SECOND_AT = {10: 0, 13: 1, 14: 2}
SLOT = {place: k for k, place in enumerate(ORDER)}
N_SLOT = len(ORDER)
N_SEND = 67
LAG = 1


def dot_nt(a, b):
    return lax.dot_general(a, b, (((1,), (1,)), ((), ())), preferred_element_type=F32)


def moe_kernel(x_ref, dy_ref, idx_ref, gain_ref, bias_ref, router_ref, wg_ref, wu_ref, wd_ref,
               y_ref, dx_ref, dgain_ref, drouter_ref, dbias_ref, dwg_ref, dwu_ref, dwd_ref,
               x_own, x_sib, part, g_own, g_sib, pg_own, pg_sib, q_buf, qg_buf,
               r1, r1g, r2, r2g, r3, r3g, r4, r4g, dl_buf, dr_buf, gn_buf, wgu, wd, acc_gu, acc_d,
               load_sem, ag_send, ag_recv, ag_grecv, sib_recv,
               rq_send, rq_recv, s1_send, s1_recv, s2_send, s2_recv, f1_send, f1_recv, f2_send, f2_recv, e_send, e_recv):
    ep = lax.axis_index("ep")
    tp = lax.axis_index("tp")
    n_tp = lax.axis_size("tp")
    n_x = lax.axis_size("ep") // 2
    core = lax.rem(ep, 2)
    chip_x = lax.div(ep, 2)
    n_loc, d_model, width = wg_ref.shape
    n_tok = x_ref.shape[0]
    n_exp = router_ref.shape[0]
    loc = n_loc * width

    def shifted(x_step, y_step):
        x_new = lax.rem(chip_x + x_step + n_x, n_x)
        y_new = lax.rem(tp + y_step + n_tp, n_tp)
        return {"tp": y_new, "ep": 2 * x_new + core}

    f_up = shifted(1 - core, core)
    f_dn = shifted(core - 1, -core)
    s_up = shifted(core, 1 - core)
    s_dn = shifted(-core, core - 1)
    f_op = shifted(2 * (1 - core), 2 * core)
    s_op = shifted(2 * core, 2 * (1 - core))
    sib = {"ep": ep + 1 - 2 * core}

    loads = []
    for e in range(n_loc):
        cols = pl.ds(e * width, width)
        loads.append(pltpu.make_async_copy(wg_ref.at[e], wgu.at[:, cols], load_sem.at[len(loads)]))
        loads.append(pltpu.make_async_copy(wu_ref.at[e], wgu.at[:, pl.ds(loc + e * width, width)], load_sem.at[len(loads)]))
        loads.append(pltpu.make_async_copy(wd_ref.at[e], wd.at[cols], load_sem.at[len(loads)]))
    for c in loads:
        c.start()
    barrier = pltpu.get_barrier_semaphore()
    peers = (f_up, f_dn, f_op, s_up, s_dn, s_op, sib)
    for dev in peers:
        pl.semaphore_signal(barrier, inc=1, device_id=dev, device_id_type=MESH)

    def normalised():
        x = x_ref[...].astype(F32)
        inv_rms = lax.rsqrt(jnp.mean(x * x, axis=-1, keepdims=True) + EPS)
        return x, inv_rms, x * inv_rms

    def chosen_mask():
        expert = lax.broadcasted_iota(jnp.int32, (n_exp, n_tok), 0)
        chosen = expert == idx_ref[0:1, :]
        for j in range(1, idx_ref.shape[0]):
            chosen = jnp.logical_or(chosen, expert == idx_ref[j:j + 1, :])
        return chosen

    gain = gain_ref[...].astype(F32).reshape(1, d_model)
    hidden = (normalised()[2] * gain).astype(BF16)
    x_own[0, 0] = hidden
    x_own[0, 1] = dy_ref[...]
    logits = jnp.where(chosen_mask(), dot_nt(router_ref[...], hidden), -jnp.inf)
    weight = jnp.exp(logits - jnp.max(logits, axis=0, keepdims=True))
    g_own[0] = weight / jnp.sum(weight, axis=0, keepdims=True)
    pl.semaphore_wait(barrier, len(peers))

    def remote(src, dst, send, recv, dev):
        return pltpu.make_async_remote_copy(src_ref=src, dst_ref=dst, send_sem=send, recv_sem=recv, device_id=dev, device_id_type=MESH)

    sends = {k: [] for k in (*range(N_SLOT), "late", "own")}
    count = [0]

    def plan(k, src, dst, recv, dev):
        n = count[0]
        count[0] += 1
        sends[k].append(lambda: remote(src, dst, ag_send.at[n], recv, dev))

    def plan_block(k, to, dev, after=None):
        after = k if after is None else after
        plan(after, x_own.at[k], x_own.at[to], ag_recv.at[to, 0], dev)
        plan(after, g_own.at[k], g_own.at[to], ag_grecv.at[to], dev)

    plan_block(0, SLOT[(3, 0)], f_up, "own")
    plan_block(0, SLOT[(1, 0)], f_dn, "own")
    for k, (df, ds) in enumerate(ORDER):
        if (df, ds) == (3, 0):
            to = SLOT[(2, 0)]
            plan(k, x_own.at[k, 0], x_own.at[to, 0], ag_recv.at[to, 0], f_up)
            plan(k, g_own.at[k], g_own.at[to], ag_grecv.at[to], f_up)
        if (df, ds) == (1, 0):
            to = SLOT[(2, 0)]
            plan(k, x_own.at[k, 1], x_own.at[to, 1], ag_recv.at[to, 1], f_dn)
        if ds == 0:
            after = "late" if (df, ds) == (3, 0) else k
            plan_block(k, SLOT[(df, 3)], s_up, after)
            plan_block(k, SLOT[(df, 1)], s_dn, after)
        if ds == 3:
            to = SLOT[(df, 2)]
            plan(k, x_own.at[k, 0], x_own.at[to, 0], ag_recv.at[to, 0], s_up)
            plan(k, g_own.at[k], g_own.at[to], ag_grecv.at[to], s_up)
        if ds == 1:
            to = SLOT[(df, 2)]
            plan(k, x_own.at[k, 1], x_own.at[to, 1], ag_recv.at[to, 1], s_dn)
        plan(k, x_own.at[k], x_sib.at[k], sib_recv.at[k, 0], sib)
        plan(k, g_own.at[k], g_sib.at[k], sib_recv.at[k, 1], sib)
    assert count[0] == N_SEND

    def arrive(k):
        if k:
            if ORDER[k][1] == 2 or ORDER[k] == (2, 0):
                for t in range(2):
                    remote(x_own.at[k, t], x_own.at[k, t], ag_send.at[0], ag_recv.at[k, t], sib).wait_recv()
            else:
                remote(x_own.at[k], x_own.at[k], ag_send.at[0], ag_recv.at[k, 0], sib).wait_recv()
            remote(g_own.at[k], g_own.at[k], ag_send.at[0], ag_grecv.at[k], sib).wait_recv()
        for make in sends[k] + (sends["late"] if ORDER[k] == (2, 0) else []):
            make().start()

    def to_sibling(k):
        return (remote(x_sib.at[k], q_buf.at[k], rq_send.at[k, 0], rq_recv.at[k, 0], sib),
                remote(pg_sib.at[k], qg_buf.at[k], rq_send.at[k, 1], rq_recv.at[k, 1], sib))

    def add_sibling(k):
        for c in to_sibling(k):
            c.wait_recv()
        part[k] = (part[k].astype(F32) + q_buf[k].astype(F32)).astype(BF16)
        pg_own[k] = pg_own[k] + qg_buf[k]

    def s_first(df):
        k = SLOT[(df, 2)]
        return (remote(part.at[k, 0], r1.at[df, 0], s1_send.at[df, 0], s1_recv.at[df, 0], s_up),
                remote(part.at[k, 1], r1.at[df, 1], s1_send.at[df, 1], s1_recv.at[df, 1], s_dn),
                remote(pg_own.at[k], r1g.at[df], s1_send.at[df, 2], s1_recv.at[df, 2], s_up))

    def s_second(df, i):
        k = SLOT[(df, (1, 3)[i])]
        dev = (s_up, s_dn)[i]
        return (remote(pg_own.at[k], r2g.at[df, i], s2_send.at[df, i, 1], s2_recv.at[df, i, 1], dev),
                remote(part.at[k], r2.at[df, i], s2_send.at[df, i, 0], s2_recv.at[df, i, 0], dev))

    def add_into(k, t, block):
        part[k, t] = (part[k, t].astype(F32) + block[...].astype(F32)).astype(BF16)

    def send_second(df):
        for c in s_first(df):
            c.wait_recv()
        k = SLOT[(df, 1)]
        add_into(k, 0, r1.at[df, 0])
        pg_own[k] = pg_own[k] + r1g[df]
        add_into(SLOT[(df, 3)], 1, r1.at[df, 1])
        for i in range(2):
            for c in s_second(df, i):
                c.start()

    row = lax.broadcasted_iota(jnp.int32, (n_exp, loc), 0)
    col = lax.broadcasted_iota(jnp.int32, (n_exp, loc), 1)
    pick = jnp.where(row == ep * n_loc + lax.div(col, width), 1.0, 0.0).astype(BF16)
    pick3 = jnp.concatenate([pick] * 3, axis=0)
    ones = jnp.ones((16, 2 * n_tok), BF16)

    def widen(g):
        hi = g.astype(BF16)
        rest = g - hi.astype(F32)
        mid = rest.astype(BF16)
        low = (rest - mid.astype(F32)).astype(BF16)
        return lax.dot_general(jnp.concatenate([hi, mid, low], axis=0), pick3, (((0,), (0,)), ((), ())), preferred_element_type=F32)

    def compute(k):
        h = jnp.concatenate([x_own[k, 0], x_sib[k, 0]], axis=0)
        dy = jnp.concatenate([x_own[k, 1], x_sib[k, 1]], axis=0)
        gate = widen(jnp.concatenate([g_own[k], g_sib[k]], axis=1))
        both = jnp.dot(h, wgu[...], preferred_element_type=F32)
        g_pre = both[:, :loc]
        u_pre = both[:, loc:]
        d_raw = dot_nt(dy, wd[...])
        used = gate != 0.0
        sig = 0.5 * jnp.tanh(0.5 * g_pre) + 0.5
        silu = g_pre * sig
        act = (silu * u_pre).astype(BF16).astype(F32)
        act_g = jnp.where(used, gate * act, 0.0).astype(BF16)
        prod = jnp.where(used, act * d_raw, 0.0)
        d_act = gate * d_raw
        d_g = jnp.where(used, d_act * u_pre * (sig + silu * (1.0 - sig)), 0.0).astype(BF16)
        d_u = jnp.where(used, d_act * silu, 0.0).astype(BF16)
        d_gu = jnp.concatenate([d_g, d_u], axis=1)
        prod_hi = prod.astype(BF16)
        prod_lo = (prod - prod_hi.astype(F32)).astype(BF16)
        dgate = dot_nt(pick, prod_hi) + dot_nt(pick, prod_lo)
        pg_own[k] = dgate[:, :n_tok]
        pg_sib[k] = dgate[:, n_tok:]
        acc_gu[...] += jnp.dot(h.T, d_gu, preferred_element_type=F32)
        acc_d[...] += jnp.dot(jnp.concatenate([act_g.T, ones], axis=0), dy, preferred_element_type=F32)
        y = jnp.dot(act_g, wd[...], preferred_element_type=F32).astype(BF16)
        part[k, 0] = y[:n_tok]
        x_sib[k, 0] = y[n_tok:]
        dh = dot_nt(d_gu, wgu[...]).astype(BF16)
        part[k, 1] = dh[:n_tok]
        x_sib[k, 1] = dh[n_tok:]

    arrive(0)
    acc_gu[...] = jnp.zeros_like(acc_gu)
    acc_d[...] = jnp.zeros_like(acc_d)
    for c in loads:
        c.wait()

    def step(k, carry):
        for j, places in ARRIVALS.items():
            @pl.when(k == j)
            def _():
                if j == 1:
                    for make in sends["own"]:
                        make().start()
                for place in places:
                    arrive(SLOT[place])
        remote(x_own.at[k], x_sib.at[k], ag_send.at[0], sib_recv.at[k, 0], sib).wait_recv()
        remote(g_own.at[k], g_sib.at[k], ag_send.at[0], sib_recv.at[k, 1], sib).wait_recv()
        compute(k)
        for c in to_sibling(k):
            c.start()

        @pl.when(k >= LAG)
        def _():
            add_sibling(k - LAG)
        for j, df in FIRST_AT.items():
            @pl.when(k == j)
            def _():
                for c in s_first(df):
                    c.start()
        for j, df in SECOND_AT.items():
            @pl.when(k == j)
            def _():
                send_second(df)
        return carry

    lax.fori_loop(0, N_SLOT, step, 0)

    stores = []
    for e in range(n_loc):
        cols = pl.ds(e * width, width)
        stores.append(pltpu.make_async_copy(acc_gu.at[:, cols], dwg_ref.at[e], load_sem.at[len(stores)]))
        stores.append(pltpu.make_async_copy(acc_gu.at[:, pl.ds(loc + e * width, width)], dwu_ref.at[e], load_sem.at[len(stores)]))
        stores.append(pltpu.make_async_copy(acc_d.at[cols], dwd_ref.at[e], load_sem.at[len(stores)]))
    for c in stores:
        c.start()
    dbias_ref[...] = acc_d[loc:loc + 1]
    for j in range(N_SLOT - LAG, N_SLOT):
        add_sibling(j)
    send_second(3)

    k2, k1, k3 = SLOT[(2, 0)], SLOT[(1, 0)], SLOT[(3, 0)]

    def wait_second(df):
        for i in range(2):
            for c in s_second(df, i):
                c.wait_recv()
        pg_own[SLOT[(df, 0)]] = pg_own[SLOT[(df, 0)]] + r2g[df, 0] + r2g[df, 1]

    def total(k, df, t):
        return part[k, t].astype(F32) + r2[df, 0, t].astype(F32) + r2[df, 1, t].astype(F32)

    f_first = (remote(pg_own.at[k2], r3g, f1_send.at[2], f1_recv.at[2], f_up),
               remote(part.at[k2, 0], r3.at[0], f1_send.at[0], f1_recv.at[0], f_up),
               remote(part.at[k2, 1], r3.at[1], f1_send.at[1], f1_recv.at[1], f_dn))
    f_second = (remote(pg_own.at[k1], r4g.at[0], f2_send.at[0], f2_recv.at[0], f_up),
                remote(pg_own.at[k3], r4g.at[1], f2_send.at[1], f2_recv.at[1], f_dn),
                remote(part.at[k1, 1], r4.at[0, 1], f2_send.at[2], f2_recv.at[2], f_up),
                remote(part.at[k3, 1], r4.at[1, 1], f2_send.at[3], f2_recv.at[3], f_dn),
                remote(part.at[k1, 0], r4.at[0, 0], f2_send.at[4], f2_recv.at[4], f_up),
                remote(part.at[k3, 0], r4.at[1, 0], f2_send.at[5], f2_recv.at[5], f_dn))
    for df, k in ((2, k2), (1, k1), (3, k3)):
        wait_second(df)
        part[k, 0] = total(k, df, 0).astype(BF16)
        part[k, 1] = total(k, df, 1).astype(BF16)
        if df == 2:
            for c in f_first:
                c.start()
        if df == 1:
            f_first[0].wait_recv()
            pg_own[k1] = pg_own[k1] + r3g[...]
            f_second[0].start()
            f_second[2].start()
            f_first[1].wait_recv()
            add_into(k1, 0, r3.at[0])
            f_second[4].start()
    f_second[1].start()
    f_first[2].wait_recv()
    add_into(k3, 1, r3.at[1])
    f_second[3].start()
    f_second[5].start()
    wait_second(0)

    for c in f_second[:2]:
        c.wait_recv()
    gates = g_own[0]
    d_gates = jnp.where(chosen_mask(), pg_own[0] + r4g[0] + r4g[1], 0.0)
    d_logits = gates * (d_gates - jnp.sum(gates * d_gates, axis=0, keepdims=True))
    dl_buf[0, 0] = d_logits
    dh_router = lax.dot_general(d_logits, router_ref[...].astype(F32), (((0,), (0,)), ((), ())), precision=lax.Precision.HIGHEST, preferred_element_type=F32)
    s_dl = [remote(dl_buf.at[0, 0], dl_buf.at[0, to], e_send.at[i], e_recv.at[i], dev) for i, (to, dev) in enumerate(((3, s_up), (1, s_dn), (2, s_op)))]
    f_dl = [remote(dl_buf.at[0], dl_buf.at[to], e_send.at[3 + i], e_recv.at[3 + i], dev) for i, (to, dev) in enumerate(((3, f_up), (1, f_dn), (2, f_op)))]
    for c in s_dl:
        c.start()

    for c in f_second[2:4]:
        c.wait_recv()
    x, inv_rms, normed = normalised()
    dh_total = total(0, 0, 1) + r4[0, 1].astype(F32) + r4[1, 1].astype(F32) + dh_router
    gn_buf[0] = jnp.sum(dh_total * normed, axis=0, keepdims=True)

    def exchange(base, group, first_sem):
        return [remote(gn_buf.at[base], gn_buf.at[base + 1 + i], e_send.at[first_sem + i], e_recv.at[first_sem + i], dev) for i, dev in enumerate(group)]

    def gathered(base, copies):
        for c in copies:
            c.wait_recv()
        summed = gn_buf[base]
        for i in range(len(copies)):
            summed = summed + gn_buf[base + 1 + i]
        return summed

    gn_sib = exchange(0, (sib,), 7)
    for c in gn_sib:
        c.start()
    for c in s_dl:
        c.wait_recv()
    for c in f_dl:
        c.start()
    d_norm = dh_total * gain
    dx_ref[...] = (dy_ref[...].astype(F32) + inv_rms * (d_norm - normed * jnp.mean(d_norm * normed, axis=-1, keepdims=True))).astype(BF16)
    gn_buf[2] = gathered(0, gn_sib)
    gn_s = exchange(2, (s_up, s_dn, s_op), 8)
    for c in gn_s:
        c.start()
    d_router = jnp.zeros((n_exp, d_model), F32)
    for c in f_dl:
        c.wait_recv()
    for k, (df, ds) in enumerate(ORDER):
        dl = dl_buf[df, ds]
        dl_hi = dl.astype(BF16)
        dl_lo = (dl - dl_hi.astype(F32)).astype(BF16)
        prods = jnp.dot(jnp.concatenate([dl_hi, dl_lo], axis=0), x_own[k, 0], preferred_element_type=F32)
        d_router = d_router + (prods[:n_exp] + prods[n_exp:])
        if k == 3:
            gn_buf[6] = gathered(2, gn_s)
            gn_f = exchange(6, (f_up, f_dn, f_op), 11)
            for c in gn_f:
                c.start()
    dr_buf[0] = d_router
    sib_dr = remote(dr_buf.at[0], dr_buf.at[1], e_send.at[6], e_recv.at[6], sib)
    sib_dr.start()
    for c in f_second[4:]:
        c.wait_recv()
    y_moe = total(0, 0, 0) + r4[0, 0].astype(F32) + r4[1, 0].astype(F32)
    y_ref[...] = (x + (y_moe + bias_ref[...].astype(F32).reshape(1, d_model))).astype(BF16)
    dgain_ref[...] = gathered(6, gn_f)
    sib_dr.wait_recv()
    drouter_ref[...] = dr_buf[0] + dr_buf[1]

    for c in f_dl + s_dl + gn_sib + gn_s + gn_f + [sib_dr]:
        c.wait_send()
    for c in stores:
        c.wait()
    for made in sends.values():
        for make in made:
            make().wait_send()
    for k in range(N_SLOT):
        for c in to_sibling(k):
            c.wait_send()
    for df in range(4):
        for c in s_first(df):
            c.wait_send()
        for i in range(2):
            for c in s_second(df, i):
                c.wait_send()
    for c in f_first + f_second:
        c.wait_send()


def moe(x, dy, idx_t, gain, bias, router_t, w_gate, w_up, w_down):
    n_tok, d_model = x.shape
    n_loc, _, width = w_gate.shape
    n_exp = router_t.shape[0]
    loc = n_loc * width
    vmem = pl.BlockSpec(memory_space=pltpu.VMEM)
    hbm = pl.BlockSpec(memory_space=pl.ANY)
    block = (2, n_tok, d_model)
    small = (n_exp, n_tok)
    dma = pltpu.SemaphoreType.DMA
    scratch = [
        pltpu.VMEM((N_SLOT, *block), BF16), pltpu.VMEM((N_SLOT, *block), BF16), pltpu.VMEM((N_SLOT, *block), BF16),
        pltpu.VMEM((N_SLOT, *small), F32), pltpu.VMEM((N_SLOT, *small), F32),
        pltpu.VMEM((N_SLOT, *small), F32), pltpu.VMEM((N_SLOT, *small), F32),
        pltpu.VMEM((N_SLOT, *block), BF16), pltpu.VMEM((N_SLOT, *small), F32),
        pltpu.VMEM((4, *block), BF16), pltpu.VMEM((4, *small), F32),
        pltpu.VMEM((4, 2, *block), BF16), pltpu.VMEM((4, 2, *small), F32),
        pltpu.VMEM(block, BF16), pltpu.VMEM(small, F32),
        pltpu.VMEM((2, *block), BF16), pltpu.VMEM((2, *small), F32),
        pltpu.VMEM((4, 4, *small), F32), pltpu.VMEM((2, n_exp, d_model), F32), pltpu.VMEM((10, 1, d_model), F32),
        pltpu.VMEM((d_model, 2 * loc), BF16), pltpu.VMEM((loc, d_model), BF16),
        pltpu.VMEM((d_model, 2 * loc), F32), pltpu.VMEM((loc + 16, d_model), F32),
        dma((3 * n_loc,)), dma((N_SEND,)), dma((N_SLOT, 2)), dma((N_SLOT,)), dma((N_SLOT, 2)),
        dma((N_SLOT, 2)), dma((N_SLOT, 2)), dma((4, 3)), dma((4, 3)), dma((4, 2, 2)), dma((4, 2, 2)),
        dma((3,)), dma((3,)), dma((6,)), dma((6,)), dma((14,)), dma((14,)),
    ]
    out_shape = (
        jax.ShapeDtypeStruct((n_tok, d_model), BF16), jax.ShapeDtypeStruct((n_tok, d_model), BF16),
        jax.ShapeDtypeStruct((1, d_model), F32), jax.ShapeDtypeStruct((n_exp, d_model), F32), jax.ShapeDtypeStruct((1, d_model), F32),
        jax.ShapeDtypeStruct(w_gate.shape, F32), jax.ShapeDtypeStruct(w_up.shape, F32), jax.ShapeDtypeStruct(w_down.shape, F32),
    )
    return pl.pallas_call(
        moe_kernel, name="moe", out_shape=out_shape,
        in_specs=[vmem] * 6 + [hbm] * 3, out_specs=(vmem,) * 5 + (hbm,) * 3,
        scratch_shapes=scratch,
        compiler_params=pltpu.CompilerParams(collective_id=0, has_side_effects=True, vmem_limit_bytes=67_043_328),
    )(x, dy, idx_t, gain, bias, router_t, w_gate, w_up, w_down)


def write_out(*refs):
    n = len(refs) // 3
    sources, results, rooms, sems = refs[:n], refs[n:2 * n], refs[2 * n:3 * n], refs[3 * n]
    pieces = []
    for i in range(n):
        for j in range(sources[i].shape[0] if len(sources[i].shape) == 3 else 1):
            at = (lambda r, j=j: r.at[j]) if len(sources[i].shape) == 3 else (lambda r: r)
            m = len(pieces)
            pieces.append((pltpu.make_async_copy(at(sources[i]), at(rooms[i]), sems.at[m, 0]),
                           pltpu.make_async_copy(at(rooms[i]), at(results[i]), sems.at[m, 1])))
    for load, _ in pieces:
        load.start()
    for load, store in pieces:
        load.wait()
        store.start()
    for _, store in pieces:
        store.wait()


def finish(*arrays):
    hbm = pl.BlockSpec(memory_space=pl.ANY)
    n_pieces = sum(a.shape[0] if a.ndim == 3 else 1 for a in arrays)
    return pl.pallas_call(
        write_out, name="finish", out_shape=tuple(jax.ShapeDtypeStruct(a.shape, a.dtype) for a in arrays),
        in_specs=[hbm] * len(arrays), out_specs=(hbm,) * len(arrays),
        scratch_shapes=[pltpu.VMEM(a.shape, a.dtype) for a in arrays] + [pltpu.SemaphoreType.DMA((n_pieces, 2))],
        compiler_params=pltpu.CompilerParams(vmem_limit_bytes=67_043_328),
    )(*arrays)


def solution(mesh):
    tok_spec = P(("dp", "ep", "tp"), None)
    wide_spec = P("ep", None, "tp")
    down_spec = P("ep", "tp", None)
    grad_wide = P(("dp", "ep"), None, "tp")
    grad_down = P(("dp", "ep"), "tp", None)

    def device_step(x_in, norm_gain, w_router, expert_idx, w_gate, w_up, w_down, out_bias, dy_out):
        y_out, dx_in, d_gain, d_router_t, d_bias, d_gate, d_up, d_down = moe(
            x_in, dy_out, expert_idx.T, norm_gain, out_bias, w_router.T, w_gate, w_up, w_down)
        y_out, dx_in, d_gate, d_up, d_down = finish(y_out, dx_in, d_gate, d_up, d_down)
        return y_out, dx_in, d_gain[0], d_router_t.T, d_gate, d_up, d_down, d_bias[0]

    return jax.shard_map(device_step, mesh=mesh, in_specs=(tok_spec, P(None), P(None, None), tok_spec, wide_spec, wide_spec, down_spec, P(None), tok_spec), out_specs=(tok_spec, tok_spec, P("dp"), P("dp", None), grad_wide, grad_wide, grad_down, P("dp")), check_vma=False)
```

```python
import jax
import jax.numpy as jnp
from jax import lax
from jax.experimental import pallas as pl
from jax.experimental.pallas import tpu as pltpu
from jax.sharding import PartitionSpec as P

EPS = 1e-6
MESH = pl.DeviceIdType.MESH
F32 = jnp.float32
BF16 = jnp.bfloat16
ORDER = ((0, 0), (0, 1), (0, 3), (0, 2), (1, 0), (1, 1), (1, 3), (2, 1), (2, 3), (3, 1), (1, 2), (2, 2), (3, 3), (3, 2), (2, 0), (3, 0))
ARRIVALS = {1: ((0, 1), (0, 3)), 2: ((1, 0), (3, 0), (0, 2)), 3: ((2, 0),), 4: ((1, 1), (1, 3)), 6: ((2, 1), (2, 3)),
            8: ((3, 1), (3, 3)), 9: ((1, 2),), 10: ((2, 2),), 11: ((3, 2),)}
FIRST_AT = {8: 0, 11: 1, 12: 2, 14: 3}
SECOND_AT = {10: 0, 13: 1, 14: 2}
SLOT = {place: k for k, place in enumerate(ORDER)}
N_SLOT = len(ORDER)
N_SEND = 67
LAG = 1


def dot_nt(a, b):
    return lax.dot_general(a, b, (((1,), (1,)), ((), ())), preferred_element_type=F32)


def moe_kernel(x_ref, dy_ref, idx_ref, gain_ref, bias_ref, router_ref, wg_ref, wu_ref, wd_ref,
               y_ref, dx_ref, dgain_ref, drouter_ref, dbias_ref, dwg_ref, dwu_ref, dwd_ref,
               x_own, x_sib, part, g_own, g_sib, pg_own, pg_sib, q_buf, qg_buf,
               r1, r1g, r2, r2g, r3, r3g, r4, r4g, dl_buf, dr_buf, gn_buf, wgu, wd, acc_gu, acc_d,
               load_sem, ag_send, ag_recv, ag_grecv, sib_recv,
               rq_send, rq_recv, s1_send, s1_recv, s2_send, s2_recv, f1_send, f1_recv, f2_send, f2_recv, e_send, e_recv):
    ep = lax.axis_index("ep")
    tp = lax.axis_index("tp")
    n_tp = lax.axis_size("tp")
    n_x = lax.axis_size("ep") // 2
    core = lax.rem(ep, 2)
    chip_x = lax.div(ep, 2)
    n_loc, d_model, width = wg_ref.shape
    n_tok = x_ref.shape[0]
    n_exp = router_ref.shape[0]
    loc = n_loc * width

    def shifted(x_step, y_step):
        x_new = lax.rem(chip_x + x_step + n_x, n_x)
        y_new = lax.rem(tp + y_step + n_tp, n_tp)
        return {"tp": y_new, "ep": 2 * x_new + core}

    f_up = shifted(1 - core, core)
    f_dn = shifted(core - 1, -core)
    s_up = shifted(core, 1 - core)
    s_dn = shifted(-core, core - 1)
    f_op = shifted(2 * (1 - core), 2 * core)
    s_op = shifted(2 * core, 2 * (1 - core))
    sib = {"ep": ep + 1 - 2 * core}

    loads = []
    for e in range(n_loc):
        cols = pl.ds(e * width, width)
        loads.append(pltpu.make_async_copy(wg_ref.at[e], wgu.at[:, cols], load_sem.at[len(loads)]))
        loads.append(pltpu.make_async_copy(wu_ref.at[e], wgu.at[:, pl.ds(loc + e * width, width)], load_sem.at[len(loads)]))
        loads.append(pltpu.make_async_copy(wd_ref.at[e], wd.at[cols], load_sem.at[len(loads)]))
    for c in loads:
        c.start()
    barrier = pltpu.get_barrier_semaphore()
    peers = (f_up, f_dn, f_op, s_up, s_dn, s_op, sib)
    for dev in peers:
        pl.semaphore_signal(barrier, inc=1, device_id=dev, device_id_type=MESH)

    def normalised():
        x = x_ref[...].astype(F32)
        inv_rms = lax.rsqrt(jnp.mean(x * x, axis=-1, keepdims=True) + EPS)
        return x, inv_rms, x * inv_rms

    def chosen_mask():
        expert = lax.broadcasted_iota(jnp.int32, (n_exp, n_tok), 0)
        chosen = expert == idx_ref[0:1, :]
        for j in range(1, idx_ref.shape[0]):
            chosen = jnp.logical_or(chosen, expert == idx_ref[j:j + 1, :])
        return chosen

    gain = gain_ref[...].astype(F32).reshape(1, d_model)
    hidden = (normalised()[2] * gain).astype(BF16)
    x_own[0, 0] = hidden
    x_own[0, 1] = dy_ref[...]
    logits = jnp.where(chosen_mask(), dot_nt(router_ref[...], hidden), -jnp.inf)
    weight = jnp.exp(logits - jnp.max(logits, axis=0, keepdims=True))
    g_own[0] = weight / jnp.sum(weight, axis=0, keepdims=True)
    pl.semaphore_wait(barrier, len(peers))

    def remote(src, dst, send, recv, dev):
        return pltpu.make_async_remote_copy(src_ref=src, dst_ref=dst, send_sem=send, recv_sem=recv, device_id=dev, device_id_type=MESH)

    sends = {k: [] for k in (*range(N_SLOT), "late", "own")}
    count = [0]

    def plan(k, src, dst, recv, dev):
        n = count[0]
        count[0] += 1
        sends[k].append(lambda: remote(src, dst, ag_send.at[n], recv, dev))

    def plan_block(k, to, dev, after=None):
        after = k if after is None else after
        plan(after, x_own.at[k], x_own.at[to], ag_recv.at[to, 0], dev)
        plan(after, g_own.at[k], g_own.at[to], ag_grecv.at[to], dev)

    plan_block(0, SLOT[(3, 0)], f_up, "own")
    plan_block(0, SLOT[(1, 0)], f_dn, "own")
    for k, (df, ds) in enumerate(ORDER):
        if (df, ds) == (3, 0):
            to = SLOT[(2, 0)]
            plan(k, x_own.at[k, 0], x_own.at[to, 0], ag_recv.at[to, 0], f_up)
            plan(k, g_own.at[k], g_own.at[to], ag_grecv.at[to], f_up)
        if (df, ds) == (1, 0):
            to = SLOT[(2, 0)]
            plan(k, x_own.at[k, 1], x_own.at[to, 1], ag_recv.at[to, 1], f_dn)
        if ds == 0:
            after = "late" if (df, ds) == (3, 0) else k
            plan_block(k, SLOT[(df, 3)], s_up, after)
            plan_block(k, SLOT[(df, 1)], s_dn, after)
        if ds == 3:
            to = SLOT[(df, 2)]
            plan(k, x_own.at[k, 0], x_own.at[to, 0], ag_recv.at[to, 0], s_up)
            plan(k, g_own.at[k], g_own.at[to], ag_grecv.at[to], s_up)
        if ds == 1:
            to = SLOT[(df, 2)]
            plan(k, x_own.at[k, 1], x_own.at[to, 1], ag_recv.at[to, 1], s_dn)
        plan(k, x_own.at[k], x_sib.at[k], sib_recv.at[k, 0], sib)
        plan(k, g_own.at[k], g_sib.at[k], sib_recv.at[k, 1], sib)
    assert count[0] == N_SEND

    def arrive(k):
        if k:
            if ORDER[k][1] == 2 or ORDER[k] == (2, 0):
                for t in range(2):
                    remote(x_own.at[k, t], x_own.at[k, t], ag_send.at[0], ag_recv.at[k, t], sib).wait_recv()
            else:
                remote(x_own.at[k], x_own.at[k], ag_send.at[0], ag_recv.at[k, 0], sib).wait_recv()
            remote(g_own.at[k], g_own.at[k], ag_send.at[0], ag_grecv.at[k], sib).wait_recv()
        for make in sends[k] + (sends["late"] if ORDER[k] == (2, 0) else []):
            make().start()

    def to_sibling(k):
        return (remote(x_sib.at[k], q_buf.at[k], rq_send.at[k, 0], rq_recv.at[k, 0], sib),
                remote(pg_sib.at[k], qg_buf.at[k], rq_send.at[k, 1], rq_recv.at[k, 1], sib))

    def add_sibling(k):
        for c in to_sibling(k):
            c.wait_recv()
        part[k] = (part[k].astype(F32) + q_buf[k].astype(F32)).astype(BF16)
        pg_own[k] = pg_own[k] + qg_buf[k]

    def s_first(df):
        k = SLOT[(df, 2)]
        return (remote(part.at[k, 0], r1.at[df, 0], s1_send.at[df, 0], s1_recv.at[df, 0], s_up),
                remote(part.at[k, 1], r1.at[df, 1], s1_send.at[df, 1], s1_recv.at[df, 1], s_dn),
                remote(pg_own.at[k], r1g.at[df], s1_send.at[df, 2], s1_recv.at[df, 2], s_up))

    def s_second(df, i):
        k = SLOT[(df, (1, 3)[i])]
        dev = (s_up, s_dn)[i]
        return (remote(pg_own.at[k], r2g.at[df, i], s2_send.at[df, i, 1], s2_recv.at[df, i, 1], dev),
                remote(part.at[k], r2.at[df, i], s2_send.at[df, i, 0], s2_recv.at[df, i, 0], dev))

    def add_into(k, t, block):
        part[k, t] = (part[k, t].astype(F32) + block[...].astype(F32)).astype(BF16)

    def send_second(df):
        for c in s_first(df):
            c.wait_recv()
        k = SLOT[(df, 1)]
        add_into(k, 0, r1.at[df, 0])
        pg_own[k] = pg_own[k] + r1g[df]
        add_into(SLOT[(df, 3)], 1, r1.at[df, 1])
        for i in range(2):
            for c in s_second(df, i):
                c.start()

    row = lax.broadcasted_iota(jnp.int32, (n_exp, loc), 0)
    col = lax.broadcasted_iota(jnp.int32, (n_exp, loc), 1)
    pick = jnp.where(row == ep * n_loc + lax.div(col, width), 1.0, 0.0).astype(BF16)
    pick3 = jnp.concatenate([pick] * 3, axis=0)
    ones = jnp.ones((16, 2 * n_tok), BF16)

    def widen(g):
        hi = g.astype(BF16)
        rest = g - hi.astype(F32)
        mid = rest.astype(BF16)
        low = (rest - mid.astype(F32)).astype(BF16)
        return lax.dot_general(jnp.concatenate([hi, mid, low], axis=0), pick3, (((0,), (0,)), ((), ())), preferred_element_type=F32)

    def compute(k):
        h = jnp.concatenate([x_own[k, 0], x_sib[k, 0]], axis=0)
        dy = jnp.concatenate([x_own[k, 1], x_sib[k, 1]], axis=0)
        gate = widen(jnp.concatenate([g_own[k], g_sib[k]], axis=1))
        both = jnp.dot(h, wgu[...], preferred_element_type=F32)
        g_pre = both[:, :loc]
        u_pre = both[:, loc:]
        d_raw = dot_nt(dy, wd[...])
        used = gate != 0.0
        sig = 0.5 * jnp.tanh(0.5 * g_pre) + 0.5
        silu = g_pre * sig
        act = (silu * u_pre).astype(BF16).astype(F32)
        act_g = jnp.where(used, gate * act, 0.0).astype(BF16)
        prod = jnp.where(used, act * d_raw, 0.0)
        d_act = gate * d_raw
        d_g = jnp.where(used, d_act * u_pre * (sig + silu * (1.0 - sig)), 0.0).astype(BF16)
        d_u = jnp.where(used, d_act * silu, 0.0).astype(BF16)
        d_gu = jnp.concatenate([d_g, d_u], axis=1)
        prod_hi = prod.astype(BF16)
        prod_lo = (prod - prod_hi.astype(F32)).astype(BF16)
        dgate = dot_nt(pick, prod_hi) + dot_nt(pick, prod_lo)
        pg_own[k] = dgate[:, :n_tok]
        pg_sib[k] = dgate[:, n_tok:]
        acc_gu[...] += jnp.dot(h.T, d_gu, preferred_element_type=F32)
        acc_d[...] += jnp.dot(jnp.concatenate([act_g.T, ones], axis=0), dy, preferred_element_type=F32)
        y = jnp.dot(act_g, wd[...], preferred_element_type=F32).astype(BF16)
        part[k, 0] = y[:n_tok]
        x_sib[k, 0] = y[n_tok:]
        dh = dot_nt(d_gu, wgu[...]).astype(BF16)
        part[k, 1] = dh[:n_tok]
        x_sib[k, 1] = dh[n_tok:]

    arrive(0)
    acc_gu[...] = jnp.zeros_like(acc_gu)
    acc_d[...] = jnp.zeros_like(acc_d)
    for c in loads:
        c.wait()

    def step(k, carry):
        for j, places in ARRIVALS.items():
            @pl.when(k == j)
            def _():
                if j == 1:
                    for make in sends["own"]:
                        make().start()
                for place in places:
                    arrive(SLOT[place])
        remote(x_own.at[k], x_sib.at[k], ag_send.at[0], sib_recv.at[k, 0], sib).wait_recv()
        remote(g_own.at[k], g_sib.at[k], ag_send.at[0], sib_recv.at[k, 1], sib).wait_recv()
        compute(k)
        for c in to_sibling(k):
            c.start()

        @pl.when(k >= LAG)
        def _():
            add_sibling(k - LAG)
        for j, df in FIRST_AT.items():
            @pl.when(k == j)
            def _():
                for c in s_first(df):
                    c.start()
        for j, df in SECOND_AT.items():
            @pl.when(k == j)
            def _():
                send_second(df)
        return carry

    lax.fori_loop(0, N_SLOT, step, 0)

    send_second(3)

    stores = []
    for e in range(n_loc):
        cols = pl.ds(e * width, width)
        stores.append(pltpu.make_async_copy(acc_gu.at[:, cols], dwg_ref.at[e], load_sem.at[len(stores)]))
        stores.append(pltpu.make_async_copy(acc_gu.at[:, pl.ds(loc + e * width, width)], dwu_ref.at[e], load_sem.at[len(stores)]))
        stores.append(pltpu.make_async_copy(acc_d.at[cols], dwd_ref.at[e], load_sem.at[len(stores)]))
    for c in stores:
        c.start()
    dbias_ref[...] = acc_d[loc:loc + 1]
    for j in range(N_SLOT - LAG, N_SLOT):
        add_sibling(j)

    k2, k1, k3 = SLOT[(2, 0)], SLOT[(1, 0)], SLOT[(3, 0)]

    def wait_second(df):
        for i in range(2):
            for c in s_second(df, i):
                c.wait_recv()
        pg_own[SLOT[(df, 0)]] = pg_own[SLOT[(df, 0)]] + r2g[df, 0] + r2g[df, 1]

    def total(k, df, t):
        return part[k, t].astype(F32) + r2[df, 0, t].astype(F32) + r2[df, 1, t].astype(F32)

    f_first = (remote(pg_own.at[k2], r3g, f1_send.at[2], f1_recv.at[2], f_up),
               remote(part.at[k2, 0], r3.at[0], f1_send.at[0], f1_recv.at[0], f_up),
               remote(part.at[k2, 1], r3.at[1], f1_send.at[1], f1_recv.at[1], f_dn))
    f_second = (remote(pg_own.at[k1], r4g.at[0], f2_send.at[0], f2_recv.at[0], f_up),
                remote(pg_own.at[k3], r4g.at[1], f2_send.at[1], f2_recv.at[1], f_dn),
                remote(part.at[k1, 1], r4.at[0, 1], f2_send.at[2], f2_recv.at[2], f_up),
                remote(part.at[k3, 1], r4.at[1, 1], f2_send.at[3], f2_recv.at[3], f_dn),
                remote(part.at[k1, 0], r4.at[0, 0], f2_send.at[4], f2_recv.at[4], f_up),
                remote(part.at[k3, 0], r4.at[1, 0], f2_send.at[5], f2_recv.at[5], f_dn))
    for df, k in ((2, k2), (1, k1), (3, k3)):
        wait_second(df)
        part[k, 0] = total(k, df, 0).astype(BF16)
        part[k, 1] = total(k, df, 1).astype(BF16)
        if df == 2:
            for c in f_first:
                c.start()
        if df == 1:
            f_first[0].wait_recv()
            pg_own[k1] = pg_own[k1] + r3g[...]
            f_second[0].start()
            f_second[2].start()
            f_first[1].wait_recv()
            add_into(k1, 0, r3.at[0])
    f_second[1].start()
    f_first[2].wait_recv()
    add_into(k3, 1, r3.at[1])
    f_second[3].start()

    gates = g_own[0]
    chosen = chosen_mask()
    x, inv_rms, normed = normalised()
    wait_second(0)
    for c in f_second[:2]:
        c.wait_recv()
    d_gates = jnp.where(chosen, pg_own[0] + r4g[0] + r4g[1], 0.0)
    d_logits = gates * (d_gates - jnp.sum(gates * d_gates, axis=0, keepdims=True))
    dl_buf[0, 0] = d_logits
    s_dl = [remote(dl_buf.at[0, 0], dl_buf.at[0, to], e_send.at[i], e_recv.at[i], dev) for i, (to, dev) in enumerate(((3, s_up), (1, s_dn), (2, s_op)))]
    f_dl = [remote(dl_buf.at[0], dl_buf.at[to], e_send.at[3 + i], e_recv.at[3 + i], dev) for i, (to, dev) in enumerate(((3, f_up), (1, f_dn), (2, f_op)))]
    for c in s_dl:
        c.start()
    dh_router = lax.dot_general(d_logits, router_ref[...].astype(F32), (((0,), (0,)), ((), ())), precision=lax.Precision.HIGHEST, preferred_element_type=F32)
    for c in s_dl:
        c.wait_recv()
    for c in f_dl:
        c.start()
    f_second[4].start()
    f_second[5].start()

    for c in f_second[2:4]:
        c.wait_recv()
    dh_total = total(0, 0, 1) + r4[0, 1].astype(F32) + r4[1, 1].astype(F32) + dh_router
    gn_buf[0] = jnp.sum(dh_total * normed, axis=0, keepdims=True)

    def exchange(base, group, first_sem):
        return [remote(gn_buf.at[base], gn_buf.at[base + 1 + i], e_send.at[first_sem + i], e_recv.at[first_sem + i], dev) for i, dev in enumerate(group)]

    def gathered(base, copies):
        for c in copies:
            c.wait_recv()
        summed = gn_buf[base]
        for i in range(len(copies)):
            summed = summed + gn_buf[base + 1 + i]
        return summed

    gn_sib = exchange(0, (sib,), 7)
    for c in gn_sib:
        c.start()
    d_norm = dh_total * gain
    dx_ref[...] = (dy_ref[...].astype(F32) + inv_rms * (d_norm - normed * jnp.mean(d_norm * normed, axis=-1, keepdims=True))).astype(BF16)
    gn_buf[2] = gathered(0, gn_sib)
    gn_s = exchange(2, (s_up, s_dn, s_op), 8)
    for c in gn_s:
        c.start()
    d_router = jnp.zeros((n_exp, d_model), F32)
    for c in f_dl:
        c.wait_recv()
    for k, (df, ds) in enumerate(ORDER):
        dl = dl_buf[df, ds]
        dl_hi = dl.astype(BF16)
        dl_lo = (dl - dl_hi.astype(F32)).astype(BF16)
        prods = jnp.dot(jnp.concatenate([dl_hi, dl_lo], axis=0), x_own[k, 0], preferred_element_type=F32)
        d_router = d_router + (prods[:n_exp] + prods[n_exp:])
        if k == 3:
            gn_buf[6] = gathered(2, gn_s)
            gn_f = exchange(6, (f_up, f_dn, f_op), 11)
            for c in gn_f:
                c.start()
    dr_buf[0] = d_router
    sib_dr = remote(dr_buf.at[0], dr_buf.at[1], e_send.at[6], e_recv.at[6], sib)
    sib_dr.start()
    for c in f_second[4:]:
        c.wait_recv()
    y_moe = total(0, 0, 0) + r4[0, 0].astype(F32) + r4[1, 0].astype(F32)
    y_ref[...] = (x + (y_moe + bias_ref[...].astype(F32).reshape(1, d_model))).astype(BF16)
    dgain_ref[...] = gathered(6, gn_f)
    sib_dr.wait_recv()
    drouter_ref[...] = dr_buf[0] + dr_buf[1]

    for c in f_dl + s_dl + gn_sib + gn_s + gn_f + [sib_dr]:
        c.wait_send()
    for c in stores:
        c.wait()
    for made in sends.values():
        for make in made:
            make().wait_send()
    for k in range(N_SLOT):
        for c in to_sibling(k):
            c.wait_send()
    for df in range(4):
        for c in s_first(df):
            c.wait_send()
        for i in range(2):
            for c in s_second(df, i):
                c.wait_send()
    for c in f_first + f_second:
        c.wait_send()


def moe(x, dy, idx_t, gain, bias, router_t, w_gate, w_up, w_down):
    n_tok, d_model = x.shape
    n_loc, _, width = w_gate.shape
    n_exp = router_t.shape[0]
    loc = n_loc * width
    vmem = pl.BlockSpec(memory_space=pltpu.VMEM)
    hbm = pl.BlockSpec(memory_space=pl.ANY)
    block = (2, n_tok, d_model)
    small = (n_exp, n_tok)
    dma = pltpu.SemaphoreType.DMA
    scratch = [
        pltpu.VMEM((N_SLOT, *block), BF16), pltpu.VMEM((N_SLOT, *block), BF16), pltpu.VMEM((N_SLOT, *block), BF16),
        pltpu.VMEM((N_SLOT, *small), F32), pltpu.VMEM((N_SLOT, *small), F32),
        pltpu.VMEM((N_SLOT, *small), F32), pltpu.VMEM((N_SLOT, *small), F32),
        pltpu.VMEM((N_SLOT, *block), BF16), pltpu.VMEM((N_SLOT, *small), F32),
        pltpu.VMEM((4, *block), BF16), pltpu.VMEM((4, *small), F32),
        pltpu.VMEM((4, 2, *block), BF16), pltpu.VMEM((4, 2, *small), F32),
        pltpu.VMEM(block, BF16), pltpu.VMEM(small, F32),
        pltpu.VMEM((2, *block), BF16), pltpu.VMEM((2, *small), F32),
        pltpu.VMEM((4, 4, *small), F32), pltpu.VMEM((2, n_exp, d_model), F32), pltpu.VMEM((10, 1, d_model), F32),
        pltpu.VMEM((d_model, 2 * loc), BF16), pltpu.VMEM((loc, d_model), BF16),
        pltpu.VMEM((d_model, 2 * loc), F32), pltpu.VMEM((loc + 16, d_model), F32),
        dma((3 * n_loc,)), dma((N_SEND,)), dma((N_SLOT, 2)), dma((N_SLOT,)), dma((N_SLOT, 2)),
        dma((N_SLOT, 2)), dma((N_SLOT, 2)), dma((4, 3)), dma((4, 3)), dma((4, 2, 2)), dma((4, 2, 2)),
        dma((3,)), dma((3,)), dma((6,)), dma((6,)), dma((14,)), dma((14,)),
    ]
    out_shape = (
        jax.ShapeDtypeStruct((n_tok, d_model), BF16), jax.ShapeDtypeStruct((n_tok, d_model), BF16),
        jax.ShapeDtypeStruct((1, d_model), F32), jax.ShapeDtypeStruct((n_exp, d_model), F32), jax.ShapeDtypeStruct((1, d_model), F32),
        jax.ShapeDtypeStruct(w_gate.shape, F32), jax.ShapeDtypeStruct(w_up.shape, F32), jax.ShapeDtypeStruct(w_down.shape, F32),
    )
    return pl.pallas_call(
        moe_kernel, name="moe", out_shape=out_shape,
        in_specs=[vmem] * 6 + [hbm] * 3, out_specs=(vmem,) * 5 + (hbm,) * 3,
        scratch_shapes=scratch,
        compiler_params=pltpu.CompilerParams(collective_id=0, has_side_effects=True, vmem_limit_bytes=67_043_328),
    )(x, dy, idx_t, gain, bias, router_t, w_gate, w_up, w_down)


def write_out(*refs):
    n = len(refs) // 3
    sources, results, rooms, sems = refs[:n], refs[n:2 * n], refs[2 * n:3 * n], refs[3 * n]
    pieces = []
    for i in range(n):
        for j in range(sources[i].shape[0] if len(sources[i].shape) == 3 else 1):
            at = (lambda r, j=j: r.at[j]) if len(sources[i].shape) == 3 else (lambda r: r)
            m = len(pieces)
            pieces.append((pltpu.make_async_copy(at(sources[i]), at(rooms[i]), sems.at[m, 0]),
                           pltpu.make_async_copy(at(rooms[i]), at(results[i]), sems.at[m, 1])))
    for load, _ in pieces:
        load.start()
    for load, store in pieces:
        load.wait()
        store.start()
    for _, store in pieces:
        store.wait()


def finish(*arrays):
    hbm = pl.BlockSpec(memory_space=pl.ANY)
    n_pieces = sum(a.shape[0] if a.ndim == 3 else 1 for a in arrays)
    return pl.pallas_call(
        write_out, name="finish", out_shape=tuple(jax.ShapeDtypeStruct(a.shape, a.dtype) for a in arrays),
        in_specs=[hbm] * len(arrays), out_specs=(hbm,) * len(arrays),
        scratch_shapes=[pltpu.VMEM(a.shape, a.dtype) for a in arrays] + [pltpu.SemaphoreType.DMA((n_pieces, 2))],
        compiler_params=pltpu.CompilerParams(vmem_limit_bytes=67_043_328),
    )(*arrays)


def solution(mesh):
    tok_spec = P(("dp", "ep", "tp"), None)
    wide_spec = P("ep", None, "tp")
    down_spec = P("ep", "tp", None)
    grad_wide = P(("dp", "ep"), None, "tp")
    grad_down = P(("dp", "ep"), "tp", None)

    def device_step(x_in, norm_gain, w_router, expert_idx, w_gate, w_up, w_down, out_bias, dy_out):
        y_out, dx_in, d_gain, d_router_t, d_bias, d_gate, d_up, d_down = moe(
            x_in, dy_out, expert_idx.T, norm_gain, out_bias, w_router.T, w_gate, w_up, w_down)
        y_out, dx_in, d_gain, d_router_t, d_gate, d_up, d_down, d_bias = finish(y_out, dx_in, d_gain, d_router_t, d_gate, d_up, d_down, d_bias)
        return y_out, dx_in, d_gain[0], d_router_t.T, d_gate, d_up, d_down, d_bias[0]

    return jax.shard_map(device_step, mesh=mesh, in_specs=(tok_spec, P(None), P(None, None), tok_spec, wide_spec, wide_spec, down_spec, P(None), tok_spec), out_specs=(tok_spec, tok_spec, P("dp"), P("dp", None), grad_wide, grad_wide, grad_down, P("dp")), check_vma=False)
```

```python
import jax
import jax.numpy as jnp
from jax import lax
from jax.experimental import pallas as pl
from jax.experimental.pallas import tpu as pltpu
from jax.sharding import PartitionSpec as P

EPS = 1e-6
MESH = pl.DeviceIdType.MESH
F32 = jnp.float32
BF16 = jnp.bfloat16
ORDER = ((0, 0), (0, 1), (0, 3), (0, 2), (1, 0), (1, 1), (1, 3), (2, 1), (2, 3), (1, 2), (2, 2), (3, 1), (3, 3), (3, 2), (2, 0), (3, 0))
ARRIVALS = {1: ((0, 1), (0, 3)), 2: ((1, 0), (3, 0), (0, 2)), 3: ((2, 0),), 4: ((1, 1), (1, 3)), 6: ((2, 1), (2, 3)),
            8: ((3, 1), (3, 3), (1, 2)), 9: ((2, 2),), 11: ((3, 2),)}
FIRST_AT = {8: 0, 10: 1, 11: 2, 14: 3}
SECOND_AT = {12: 1, 13: 2}
SLOT = {place: k for k, place in enumerate(ORDER)}
N_SLOT = len(ORDER)
N_SEND = 67
LAG = 1


def dot_nt(a, b):
    return lax.dot_general(a, b, (((1,), (1,)), ((), ())), preferred_element_type=F32)


def moe_kernel(x_ref, dy_ref, idx_ref, gain_ref, bias_ref, router_ref, wg_ref, wu_ref, wd_ref,
               y_ref, dx_ref, dgain_ref, drouter_ref, dbias_ref, dwg_ref, dwu_ref, dwd_ref,
               x_own, x_sib, part, g_own, g_sib, pg_own, pg_sib, q_buf, qg_buf,
               r1, r1g, r2, r2g, r3, r3g, r4, r4g, dl_buf, dr_buf, gn_buf, wgu, wd, acc_gu, acc_d,
               load_sem, ag_send, ag_recv, ag_grecv, sib_recv,
               rq_send, rq_recv, s1_send, s1_recv, s2_send, s2_recv, f1_send, f1_recv, f2_send, f2_recv, e_send, e_recv):
    ep = lax.axis_index("ep")
    tp = lax.axis_index("tp")
    n_tp = lax.axis_size("tp")
    n_x = lax.axis_size("ep") // 2
    core = lax.rem(ep, 2)
    chip_x = lax.div(ep, 2)
    n_loc, d_model, width = wg_ref.shape
    n_tok = x_ref.shape[0]
    n_exp = router_ref.shape[0]
    loc = n_loc * width

    def shifted(x_step, y_step):
        x_new = lax.rem(chip_x + x_step + n_x, n_x)
        y_new = lax.rem(tp + y_step + n_tp, n_tp)
        return {"tp": y_new, "ep": 2 * x_new + core}

    f_up = shifted(1 - core, core)
    f_dn = shifted(core - 1, -core)
    s_up = shifted(core, 1 - core)
    s_dn = shifted(-core, core - 1)
    f_op = shifted(2 * (1 - core), 2 * core)
    s_op = shifted(2 * core, 2 * (1 - core))
    sib = {"ep": ep + 1 - 2 * core}

    loads = []
    for e in range(n_loc):
        cols = pl.ds(e * width, width)
        loads.append(pltpu.make_async_copy(wg_ref.at[e], wgu.at[:, cols], load_sem.at[len(loads)]))
        loads.append(pltpu.make_async_copy(wu_ref.at[e], wgu.at[:, pl.ds(loc + e * width, width)], load_sem.at[len(loads)]))
        loads.append(pltpu.make_async_copy(wd_ref.at[e], wd.at[cols], load_sem.at[len(loads)]))
    for c in loads:
        c.start()
    barrier = pltpu.get_barrier_semaphore()
    peers = (f_up, f_dn, f_op, s_up, s_dn, s_op, sib)
    for dev in peers:
        pl.semaphore_signal(barrier, inc=1, device_id=dev, device_id_type=MESH)

    def normalised():
        x = x_ref[...].astype(F32)
        inv_rms = lax.rsqrt(jnp.mean(x * x, axis=-1, keepdims=True) + EPS)
        return x, inv_rms, x * inv_rms

    def chosen_mask():
        expert = lax.broadcasted_iota(jnp.int32, (n_exp, n_tok), 0)
        chosen = expert == idx_ref[0:1, :]
        for j in range(1, idx_ref.shape[0]):
            chosen = jnp.logical_or(chosen, expert == idx_ref[j:j + 1, :])
        return chosen

    gain = gain_ref[...].astype(F32).reshape(1, d_model)
    hidden = (normalised()[2] * gain).astype(BF16)
    x_own[0, 0] = hidden
    x_own[0, 1] = dy_ref[...]
    logits = jnp.where(chosen_mask(), dot_nt(router_ref[...], hidden), -jnp.inf)
    weight = jnp.exp(logits - jnp.max(logits, axis=0, keepdims=True))
    g_own[0] = weight / jnp.sum(weight, axis=0, keepdims=True)
    pl.semaphore_wait(barrier, len(peers))

    def remote(src, dst, send, recv, dev):
        return pltpu.make_async_remote_copy(src_ref=src, dst_ref=dst, send_sem=send, recv_sem=recv, device_id=dev, device_id_type=MESH)

    sends = {k: [] for k in (*range(N_SLOT), "late", "own")}
    count = [0]

    def plan(k, src, dst, recv, dev):
        n = count[0]
        count[0] += 1
        sends[k].append(lambda: remote(src, dst, ag_send.at[n], recv, dev))

    def plan_block(k, to, dev, after=None):
        after = k if after is None else after
        plan(after, x_own.at[k], x_own.at[to], ag_recv.at[to, 0], dev)
        plan(after, g_own.at[k], g_own.at[to], ag_grecv.at[to], dev)

    plan_block(0, SLOT[(3, 0)], f_up, "own")
    plan_block(0, SLOT[(1, 0)], f_dn, "own")
    for k, (df, ds) in enumerate(ORDER):
        if (df, ds) == (3, 0):
            to = SLOT[(2, 0)]
            plan(k, x_own.at[k, 0], x_own.at[to, 0], ag_recv.at[to, 0], f_up)
            plan(k, g_own.at[k], g_own.at[to], ag_grecv.at[to], f_up)
        if (df, ds) == (1, 0):
            to = SLOT[(2, 0)]
            plan(k, x_own.at[k, 1], x_own.at[to, 1], ag_recv.at[to, 1], f_dn)
        if ds == 0:
            after = "late" if (df, ds) == (3, 0) else k
            plan_block(k, SLOT[(df, 3)], s_up, after)
            plan_block(k, SLOT[(df, 1)], s_dn, after)
        if ds == 3:
            to = SLOT[(df, 2)]
            plan(k, x_own.at[k, 0], x_own.at[to, 0], ag_recv.at[to, 0], s_up)
            plan(k, g_own.at[k], g_own.at[to], ag_grecv.at[to], s_up)
        if ds == 1:
            to = SLOT[(df, 2)]
            plan(k, x_own.at[k, 1], x_own.at[to, 1], ag_recv.at[to, 1], s_dn)
        plan(k, x_own.at[k], x_sib.at[k], sib_recv.at[k, 0], sib)
        plan(k, g_own.at[k], g_sib.at[k], sib_recv.at[k, 1], sib)
    assert count[0] == N_SEND

    def arrive(k):
        if k:
            if ORDER[k][1] == 2 or ORDER[k] == (2, 0):
                for t in range(2):
                    remote(x_own.at[k, t], x_own.at[k, t], ag_send.at[0], ag_recv.at[k, t], sib).wait_recv()
            else:
                remote(x_own.at[k], x_own.at[k], ag_send.at[0], ag_recv.at[k, 0], sib).wait_recv()
            remote(g_own.at[k], g_own.at[k], ag_send.at[0], ag_grecv.at[k], sib).wait_recv()
        for make in sends[k] + (sends["late"] if ORDER[k] == (2, 0) else []):
            make().start()

    def to_sibling(k):
        return (remote(x_sib.at[k], q_buf.at[k], rq_send.at[k, 0], rq_recv.at[k, 0], sib),
                remote(pg_sib.at[k], qg_buf.at[k], rq_send.at[k, 1], rq_recv.at[k, 1], sib))

    def add_sibling(k):
        for c in to_sibling(k):
            c.wait_recv()
        part[k] = (part[k].astype(F32) + q_buf[k].astype(F32)).astype(BF16)
        pg_own[k] = pg_own[k] + qg_buf[k]

    def s_first(df):
        k = SLOT[(df, 2)]
        return (remote(part.at[k, 0], r1.at[df, 0], s1_send.at[df, 0], s1_recv.at[df, 0], s_up),
                remote(part.at[k, 1], r1.at[df, 1], s1_send.at[df, 1], s1_recv.at[df, 1], s_dn),
                remote(pg_own.at[k], r1g.at[df], s1_send.at[df, 2], s1_recv.at[df, 2], s_up))

    def s_second(df, i):
        k = SLOT[(df, (1, 3)[i])]
        dev = (s_up, s_dn)[i]
        return (remote(pg_own.at[k], r2g.at[df, i], s2_send.at[df, i, 1], s2_recv.at[df, i, 1], dev),
                remote(part.at[k], r2.at[df, i], s2_send.at[df, i, 0], s2_recv.at[df, i, 0], dev))

    def add_into(k, t, block):
        part[k, t] = (part[k, t].astype(F32) + block[...].astype(F32)).astype(BF16)

    def send_second(df):
        for c in s_first(df):
            c.wait_recv()
        k = SLOT[(df, 1)]
        add_into(k, 0, r1.at[df, 0])
        pg_own[k] = pg_own[k] + r1g[df]
        add_into(SLOT[(df, 3)], 1, r1.at[df, 1])
        for i in range(2):
            for c in s_second(df, i):
                c.start()

    row = lax.broadcasted_iota(jnp.int32, (n_exp, loc), 0)
    col = lax.broadcasted_iota(jnp.int32, (n_exp, loc), 1)
    pick = jnp.where(row == ep * n_loc + lax.div(col, width), 1.0, 0.0).astype(BF16)
    pick3 = jnp.concatenate([pick] * 3, axis=0)
    ones = jnp.ones((16, 2 * n_tok), BF16)

    def widen(g):
        hi = g.astype(BF16)
        rest = g - hi.astype(F32)
        mid = rest.astype(BF16)
        low = (rest - mid.astype(F32)).astype(BF16)
        return lax.dot_general(jnp.concatenate([hi, mid, low], axis=0), pick3, (((0,), (0,)), ((), ())), preferred_element_type=F32)

    def compute(k):
        h = jnp.concatenate([x_own[k, 0], x_sib[k, 0]], axis=0)
        dy = jnp.concatenate([x_own[k, 1], x_sib[k, 1]], axis=0)
        gate = widen(jnp.concatenate([g_own[k], g_sib[k]], axis=1))
        both = jnp.dot(h, wgu[...], preferred_element_type=F32)
        g_pre = both[:, :loc]
        u_pre = both[:, loc:]
        d_raw = dot_nt(dy, wd[...])
        used = gate != 0.0
        sig = 0.5 * jnp.tanh(0.5 * g_pre) + 0.5
        silu = g_pre * sig
        act = (silu * u_pre).astype(BF16).astype(F32)
        act_g = jnp.where(used, gate * act, 0.0).astype(BF16)
        prod = jnp.where(used, act * d_raw, 0.0)
        d_act = gate * d_raw
        d_g = jnp.where(used, d_act * u_pre * (sig + silu * (1.0 - sig)), 0.0).astype(BF16)
        d_u = jnp.where(used, d_act * silu, 0.0).astype(BF16)
        d_gu = jnp.concatenate([d_g, d_u], axis=1)
        prod_hi = prod.astype(BF16)
        prod_lo = (prod - prod_hi.astype(F32)).astype(BF16)
        dgate = dot_nt(pick, prod_hi) + dot_nt(pick, prod_lo)
        pg_own[k] = dgate[:, :n_tok]
        pg_sib[k] = dgate[:, n_tok:]
        acc_gu[...] += jnp.dot(h.T, d_gu, preferred_element_type=F32)
        acc_d[...] += jnp.dot(jnp.concatenate([act_g.T, ones], axis=0), dy, preferred_element_type=F32)
        y = jnp.dot(act_g, wd[...], preferred_element_type=F32).astype(BF16)
        part[k, 0] = y[:n_tok]
        x_sib[k, 0] = y[n_tok:]
        dh = dot_nt(d_gu, wgu[...]).astype(BF16)
        part[k, 1] = dh[:n_tok]
        x_sib[k, 1] = dh[n_tok:]

    arrive(0)
    acc_gu[...] = jnp.zeros_like(acc_gu)
    acc_d[...] = jnp.zeros_like(acc_d)
    for c in loads:
        c.wait()

    def step(k, carry):
        for j, places in ARRIVALS.items():
            @pl.when(k == j)
            def _():
                if j == 1:
                    for make in sends["own"]:
                        make().start()
                for place in places:
                    arrive(SLOT[place])
        remote(x_own.at[k], x_sib.at[k], ag_send.at[0], sib_recv.at[k, 0], sib).wait_recv()
        remote(g_own.at[k], g_sib.at[k], ag_send.at[0], sib_recv.at[k, 1], sib).wait_recv()
        compute(k)
        for c in to_sibling(k):
            c.start()

        @pl.when(k >= LAG)
        def _():
            add_sibling(k - LAG)
        for j, df in FIRST_AT.items():
            @pl.when(k == j)
            def _():
                for c in s_first(df):
                    c.start()
        for j, df in SECOND_AT.items():
            @pl.when(k == j)
            def _():
                send_second(df)
        return carry

    lax.fori_loop(0, N_SLOT, step, 0)

    send_second(3)

    k2, k1, k3 = SLOT[(2, 0)], SLOT[(1, 0)], SLOT[(3, 0)]

    def wait_second(df):
        for i in range(2):
            for c in s_second(df, i):
                c.wait_recv()
        pg_own[SLOT[(df, 0)]] = pg_own[SLOT[(df, 0)]] + r2g[df, 0] + r2g[df, 1]

    def total(k, df, t):
        return part[k, t].astype(F32) + r2[df, 0, t].astype(F32) + r2[df, 1, t].astype(F32)

    f_first = (remote(pg_own.at[k2], r3g, f1_send.at[2], f1_recv.at[2], f_up),
               remote(part.at[k2, 0], r3.at[0], f1_send.at[0], f1_recv.at[0], f_up),
               remote(part.at[k2, 1], r3.at[1], f1_send.at[1], f1_recv.at[1], f_dn))
    f_second = (remote(pg_own.at[k1], r4g.at[0], f2_send.at[0], f2_recv.at[0], f_up),
                remote(pg_own.at[k3], r4g.at[1], f2_send.at[1], f2_recv.at[1], f_dn),
                remote(part.at[k1, 1], r4.at[0, 1], f2_send.at[2], f2_recv.at[2], f_up),
                remote(part.at[k3, 1], r4.at[1, 1], f2_send.at[3], f2_recv.at[3], f_dn),
                remote(part.at[k1, 0], r4.at[0, 0], f2_send.at[4], f2_recv.at[4], f_up),
                remote(part.at[k3, 0], r4.at[1, 0], f2_send.at[5], f2_recv.at[5], f_dn))
    for df, k in ((2, k2), (1, k1), (3, k3)):
        wait_second(df)
        part[k, 0] = total(k, df, 0).astype(BF16)
        part[k, 1] = total(k, df, 1).astype(BF16)
        if df == 2:
            for c in f_first:
                c.start()
            send_second(0)
            stores = []
            for e in range(n_loc):
                cols = pl.ds(e * width, width)
                stores.append(pltpu.make_async_copy(acc_gu.at[:, cols], dwg_ref.at[e], load_sem.at[len(stores)]))
                stores.append(pltpu.make_async_copy(acc_gu.at[:, pl.ds(loc + e * width, width)], dwu_ref.at[e], load_sem.at[len(stores)]))
                stores.append(pltpu.make_async_copy(acc_d.at[cols], dwd_ref.at[e], load_sem.at[len(stores)]))
            for c in stores:
                c.start()
            dbias_ref[...] = acc_d[loc:loc + 1]
            for j in range(N_SLOT - LAG, N_SLOT):
                add_sibling(j)
        if df == 1:
            f_first[0].wait_recv()
            pg_own[k1] = pg_own[k1] + r3g[...]
            f_second[0].start()
            f_second[2].start()
            f_first[1].wait_recv()
            add_into(k1, 0, r3.at[0])
    f_second[1].start()
    f_first[2].wait_recv()
    add_into(k3, 1, r3.at[1])
    f_second[3].start()

    gates = g_own[0]
    chosen = chosen_mask()
    x, inv_rms, normed = normalised()
    wait_second(0)
    for c in f_second[:2]:
        c.wait_recv()
    d_gates = jnp.where(chosen, pg_own[0] + r4g[0] + r4g[1], 0.0)
    d_logits = gates * (d_gates - jnp.sum(gates * d_gates, axis=0, keepdims=True))
    dl_buf[0, 0] = d_logits
    s_dl = [remote(dl_buf.at[0, 0], dl_buf.at[0, to], e_send.at[i], e_recv.at[i], dev) for i, (to, dev) in enumerate(((3, s_up), (1, s_dn), (2, s_op)))]
    f_dl = [remote(dl_buf.at[0], dl_buf.at[to], e_send.at[3 + i], e_recv.at[3 + i], dev) for i, (to, dev) in enumerate(((3, f_up), (1, f_dn), (2, f_op)))]
    for c in s_dl:
        c.start()
    dh_router = lax.dot_general(d_logits, router_ref[...].astype(F32), (((0,), (0,)), ((), ())), precision=lax.Precision.HIGHEST, preferred_element_type=F32)
    for c in s_dl:
        c.wait_recv()
    for c in f_dl:
        c.start()
    f_second[4].start()
    f_second[5].start()

    for c in f_second[2:4]:
        c.wait_recv()
    dh_total = total(0, 0, 1) + r4[0, 1].astype(F32) + r4[1, 1].astype(F32) + dh_router
    gn_buf[0] = jnp.sum(dh_total * normed, axis=0, keepdims=True)

    def exchange(base, group, first_sem):
        return [remote(gn_buf.at[base], gn_buf.at[base + 1 + i], e_send.at[first_sem + i], e_recv.at[first_sem + i], dev) for i, dev in enumerate(group)]

    def gathered(base, copies):
        for c in copies:
            c.wait_recv()
        summed = gn_buf[base]
        for i in range(len(copies)):
            summed = summed + gn_buf[base + 1 + i]
        return summed

    gn_sib = exchange(0, (sib,), 7)
    for c in gn_sib:
        c.start()
    d_norm = dh_total * gain
    dx_ref[...] = (dy_ref[...].astype(F32) + inv_rms * (d_norm - normed * jnp.mean(d_norm * normed, axis=-1, keepdims=True))).astype(BF16)
    gn_buf[2] = gathered(0, gn_sib)
    gn_s = exchange(2, (s_up, s_dn, s_op), 8)
    for c in gn_s:
        c.start()
    d_router = jnp.zeros((n_exp, d_model), F32)
    for c in f_dl:
        c.wait_recv()
    for k, (df, ds) in enumerate(ORDER):
        dl = dl_buf[df, ds]
        dl_hi = dl.astype(BF16)
        dl_lo = (dl - dl_hi.astype(F32)).astype(BF16)
        prods = jnp.dot(jnp.concatenate([dl_hi, dl_lo], axis=0), x_own[k, 0], preferred_element_type=F32)
        d_router = d_router + (prods[:n_exp] + prods[n_exp:])
        if k == 3:
            gn_buf[6] = gathered(2, gn_s)
            gn_f = exchange(6, (f_up, f_dn, f_op), 11)
            for c in gn_f:
                c.start()
    dr_buf[0] = d_router
    sib_dr = remote(dr_buf.at[0], dr_buf.at[1], e_send.at[6], e_recv.at[6], sib)
    sib_dr.start()
    for c in f_second[4:]:
        c.wait_recv()
    y_moe = total(0, 0, 0) + r4[0, 0].astype(F32) + r4[1, 0].astype(F32)
    y_ref[...] = (x + (y_moe + bias_ref[...].astype(F32).reshape(1, d_model))).astype(BF16)
    dgain_ref[...] = gathered(6, gn_f)
    sib_dr.wait_recv()
    drouter_ref[...] = dr_buf[0] + dr_buf[1]

    for c in f_dl + s_dl + gn_sib + gn_s + gn_f + [sib_dr]:
        c.wait_send()
    for c in stores:
        c.wait()
    for made in sends.values():
        for make in made:
            make().wait_send()
    for k in range(N_SLOT):
        for c in to_sibling(k):
            c.wait_send()
    for df in range(4):
        for c in s_first(df):
            c.wait_send()
        for i in range(2):
            for c in s_second(df, i):
                c.wait_send()
    for c in f_first + f_second:
        c.wait_send()


def moe(x, dy, idx_t, gain, bias, router_t, w_gate, w_up, w_down):
    n_tok, d_model = x.shape
    n_loc, _, width = w_gate.shape
    n_exp = router_t.shape[0]
    loc = n_loc * width
    vmem = pl.BlockSpec(memory_space=pltpu.VMEM)
    hbm = pl.BlockSpec(memory_space=pl.ANY)
    block = (2, n_tok, d_model)
    small = (n_exp, n_tok)
    dma = pltpu.SemaphoreType.DMA
    scratch = [
        pltpu.VMEM((N_SLOT, *block), BF16), pltpu.VMEM((N_SLOT, *block), BF16), pltpu.VMEM((N_SLOT, *block), BF16),
        pltpu.VMEM((N_SLOT, *small), F32), pltpu.VMEM((N_SLOT, *small), F32),
        pltpu.VMEM((N_SLOT, *small), F32), pltpu.VMEM((N_SLOT, *small), F32),
        pltpu.VMEM((N_SLOT, *block), BF16), pltpu.VMEM((N_SLOT, *small), F32),
        pltpu.VMEM((4, *block), BF16), pltpu.VMEM((4, *small), F32),
        pltpu.VMEM((4, 2, *block), BF16), pltpu.VMEM((4, 2, *small), F32),
        pltpu.VMEM(block, BF16), pltpu.VMEM(small, F32),
        pltpu.VMEM((2, *block), BF16), pltpu.VMEM((2, *small), F32),
        pltpu.VMEM((4, 4, *small), F32), pltpu.VMEM((2, n_exp, d_model), F32), pltpu.VMEM((10, 1, d_model), F32),
        pltpu.VMEM((d_model, 2 * loc), BF16), pltpu.VMEM((loc, d_model), BF16),
        pltpu.VMEM((d_model, 2 * loc), F32), pltpu.VMEM((loc + 16, d_model), F32),
        dma((3 * n_loc,)), dma((N_SEND,)), dma((N_SLOT, 2)), dma((N_SLOT,)), dma((N_SLOT, 2)),
        dma((N_SLOT, 2)), dma((N_SLOT, 2)), dma((4, 3)), dma((4, 3)), dma((4, 2, 2)), dma((4, 2, 2)),
        dma((3,)), dma((3,)), dma((6,)), dma((6,)), dma((14,)), dma((14,)),
    ]
    out_shape = (
        jax.ShapeDtypeStruct((n_tok, d_model), BF16), jax.ShapeDtypeStruct((n_tok, d_model), BF16),
        jax.ShapeDtypeStruct((1, d_model), F32), jax.ShapeDtypeStruct((n_exp, d_model), F32), jax.ShapeDtypeStruct((1, d_model), F32),
        jax.ShapeDtypeStruct(w_gate.shape, F32), jax.ShapeDtypeStruct(w_up.shape, F32), jax.ShapeDtypeStruct(w_down.shape, F32),
    )
    return pl.pallas_call(
        moe_kernel, name="moe", out_shape=out_shape,
        in_specs=[vmem] * 6 + [hbm] * 3, out_specs=(vmem,) * 5 + (hbm,) * 3,
        scratch_shapes=scratch,
        compiler_params=pltpu.CompilerParams(collective_id=0, has_side_effects=True, vmem_limit_bytes=67_043_328),
    )(x, dy, idx_t, gain, bias, router_t, w_gate, w_up, w_down)


def write_out(*refs):
    n = len(refs) // 3
    sources, results, rooms, sems = refs[:n], refs[n:2 * n], refs[2 * n:3 * n], refs[3 * n]
    pieces = []
    for i in range(n):
        for j in range(sources[i].shape[0] if len(sources[i].shape) == 3 else 1):
            at = (lambda r, j=j: r.at[j]) if len(sources[i].shape) == 3 else (lambda r: r)
            m = len(pieces)
            pieces.append((pltpu.make_async_copy(at(sources[i]), at(rooms[i]), sems.at[m, 0]),
                           pltpu.make_async_copy(at(rooms[i]), at(results[i]), sems.at[m, 1])))
    for load, _ in pieces:
        load.start()
    for load, store in pieces:
        load.wait()
        store.start()
    for _, store in pieces:
        store.wait()


def finish(*arrays):
    hbm = pl.BlockSpec(memory_space=pl.ANY)
    n_pieces = sum(a.shape[0] if a.ndim == 3 else 1 for a in arrays)
    return pl.pallas_call(
        write_out, name="finish", out_shape=tuple(jax.ShapeDtypeStruct(a.shape, a.dtype) for a in arrays),
        in_specs=[hbm] * len(arrays), out_specs=(hbm,) * len(arrays),
        scratch_shapes=[pltpu.VMEM(a.shape, a.dtype) for a in arrays] + [pltpu.SemaphoreType.DMA((n_pieces, 2))],
        compiler_params=pltpu.CompilerParams(vmem_limit_bytes=67_043_328),
    )(*arrays)


def solution(mesh):
    tok_spec = P(("dp", "ep", "tp"), None)
    wide_spec = P("ep", None, "tp")
    down_spec = P("ep", "tp", None)
    grad_wide = P(("dp", "ep"), None, "tp")
    grad_down = P(("dp", "ep"), "tp", None)

    def device_step(x_in, norm_gain, w_router, expert_idx, w_gate, w_up, w_down, out_bias, dy_out):
        y_out, dx_in, d_gain, d_router_t, d_bias, d_gate, d_up, d_down = moe(
            x_in, dy_out, expert_idx.T, norm_gain, out_bias, w_router.T, w_gate, w_up, w_down)
        y_out, dx_in, d_gain, d_router_t, d_gate, d_up, d_down, d_bias = finish(y_out, dx_in, d_gain, d_router_t, d_gate, d_up, d_down, d_bias)
        return y_out, dx_in, d_gain[0], d_router_t.T, d_gate, d_up, d_down, d_bias[0]

    return jax.shard_map(device_step, mesh=mesh, in_specs=(tok_spec, P(None), P(None, None), tok_spec, wide_spec, wide_spec, down_spec, P(None), tok_spec), out_specs=(tok_spec, tok_spec, P("dp"), P("dp", None), grad_wide, grad_wide, grad_down, P("dp")), check_vma=False)
```

```python
import jax
import jax.numpy as jnp
from jax import lax
from jax.experimental import pallas as pl
from jax.experimental.pallas import tpu as pltpu
from jax.sharding import PartitionSpec as P

EPS = 1e-6
MESH = pl.DeviceIdType.MESH
F32 = jnp.float32
BF16 = jnp.bfloat16
ORDER = ((0, 0), (0, 1), (0, 3), (0, 2), (1, 0), (1, 1), (1, 3), (2, 1), (2, 3), (3, 1), (1, 2), (2, 2), (3, 3), (3, 2), (2, 0), (3, 0))
ARRIVALS = {1: ((0, 1), (0, 3)), 2: ((1, 0), (3, 0), (0, 2)), 3: ((2, 0),), 4: ((1, 1), (1, 3)), 6: ((2, 1), (2, 3)),
            8: ((3, 1), (3, 3)), 9: ((1, 2),), 10: ((2, 2),), 11: ((3, 2),)}
FIRST_AT = {8: 0, 11: 1, 12: 2, 14: 3}
SECOND_AT = {10: 0, 13: 1, 14: 2}
SLOT = {place: k for k, place in enumerate(ORDER)}
N_SLOT = len(ORDER)
N_SEND = 67
LAG = 1


def dot_nt(a, b):
    return lax.dot_general(a, b, (((1,), (1,)), ((), ())), preferred_element_type=F32)


def moe_kernel(x_ref, dy_ref, idx_ref, gain_ref, bias_ref, router_ref, wg_ref, wu_ref, wd_ref,
               y_ref, dx_ref, dgain_ref, drouter_ref, dbias_ref, dwg_ref, dwu_ref, dwd_ref,
               x_own, x_sib, part, g_own, g_sib, pg_own, pg_sib, q_buf, qg_buf,
               r1, r1g, r2, r2g, r3, r3g, r4, r4g, dl_buf, dr_buf, gn_buf, wgu, wd, acc_gu, acc_d,
               load_sem, ag_send, ag_recv, ag_grecv, sib_recv,
               rq_send, rq_recv, s1_send, s1_recv, s2_send, s2_recv, f1_send, f1_recv, f2_send, f2_recv, e_send, e_recv):
    ep = lax.axis_index("ep")
    tp = lax.axis_index("tp")
    n_tp = lax.axis_size("tp")
    n_x = lax.axis_size("ep") // 2
    core = lax.rem(ep, 2)
    chip_x = lax.div(ep, 2)
    n_loc, d_model, width = wg_ref.shape
    n_tok = x_ref.shape[0]
    n_exp = router_ref.shape[0]
    loc = n_loc * width

    def shifted(x_step, y_step):
        x_new = lax.rem(chip_x + x_step + n_x, n_x)
        y_new = lax.rem(tp + y_step + n_tp, n_tp)
        return {"tp": y_new, "ep": 2 * x_new + core}

    f_up = shifted(1 - core, core)
    f_dn = shifted(core - 1, -core)
    s_up = shifted(core, 1 - core)
    s_dn = shifted(-core, core - 1)
    f_op = shifted(2 * (1 - core), 2 * core)
    s_op = shifted(2 * core, 2 * (1 - core))
    sib = {"ep": ep + 1 - 2 * core}

    loads = []
    for e in range(n_loc):
        cols = pl.ds(e * width, width)
        loads.append(pltpu.make_async_copy(wg_ref.at[e], wgu.at[:, cols], load_sem.at[len(loads)]))
        loads.append(pltpu.make_async_copy(wu_ref.at[e], wgu.at[:, pl.ds(loc + e * width, width)], load_sem.at[len(loads)]))
        loads.append(pltpu.make_async_copy(wd_ref.at[e], wd.at[cols], load_sem.at[len(loads)]))
    for c in loads:
        c.start()
    barrier = pltpu.get_barrier_semaphore()
    peers = (f_up, f_dn, f_op, s_up, s_dn, s_op, sib)
    for dev in peers:
        pl.semaphore_signal(barrier, inc=1, device_id=dev, device_id_type=MESH)

    def normalised():
        x = x_ref[...].astype(F32)
        inv_rms = lax.rsqrt(jnp.mean(x * x, axis=-1, keepdims=True) + EPS)
        return x, inv_rms, x * inv_rms

    def chosen_mask():
        expert = lax.broadcasted_iota(jnp.int32, (n_exp, n_tok), 0)
        chosen = expert == idx_ref[0:1, :]
        for j in range(1, idx_ref.shape[0]):
            chosen = jnp.logical_or(chosen, expert == idx_ref[j:j + 1, :])
        return chosen

    gain = gain_ref[...].astype(F32).reshape(1, d_model)
    hidden = (normalised()[2] * gain).astype(BF16)
    x_own[0, 0] = hidden
    x_own[0, 1] = dy_ref[...]
    logits = jnp.where(chosen_mask(), dot_nt(router_ref[...], hidden), -jnp.inf)
    weight = jnp.exp(logits - jnp.max(logits, axis=0, keepdims=True))
    g_own[0] = weight / jnp.sum(weight, axis=0, keepdims=True)
    pl.semaphore_wait(barrier, len(peers))

    def remote(src, dst, send, recv, dev):
        return pltpu.make_async_remote_copy(src_ref=src, dst_ref=dst, send_sem=send, recv_sem=recv, device_id=dev, device_id_type=MESH)

    sends = {k: [] for k in (*range(N_SLOT), "late", "own")}
    count = [0]

    def plan(k, src, dst, recv, dev):
        n = count[0]
        count[0] += 1
        sends[k].append(lambda: remote(src, dst, ag_send.at[n], recv, dev))

    def plan_block(k, to, dev, after=None):
        after = k if after is None else after
        plan(after, x_own.at[k], x_own.at[to], ag_recv.at[to, 0], dev)
        plan(after, g_own.at[k], g_own.at[to], ag_grecv.at[to], dev)

    plan_block(0, SLOT[(3, 0)], f_up, "own")
    plan_block(0, SLOT[(1, 0)], f_dn, "own")
    for k, (df, ds) in enumerate(ORDER):
        if (df, ds) == (3, 0):
            to = SLOT[(2, 0)]
            plan(k, x_own.at[k, 0], x_own.at[to, 0], ag_recv.at[to, 0], f_up)
            plan(k, g_own.at[k], g_own.at[to], ag_grecv.at[to], f_up)
        if (df, ds) == (1, 0):
            to = SLOT[(2, 0)]
            plan(k, x_own.at[k, 1], x_own.at[to, 1], ag_recv.at[to, 1], f_dn)
        if ds == 0:
            after = "late" if (df, ds) == (3, 0) else k
            plan_block(k, SLOT[(df, 3)], s_up, after)
            plan_block(k, SLOT[(df, 1)], s_dn, after)
        if ds == 3:
            to = SLOT[(df, 2)]
            plan(k, x_own.at[k, 0], x_own.at[to, 0], ag_recv.at[to, 0], s_up)
            plan(k, g_own.at[k], g_own.at[to], ag_grecv.at[to], s_up)
        if ds == 1:
            to = SLOT[(df, 2)]
            plan(k, x_own.at[k, 1], x_own.at[to, 1], ag_recv.at[to, 1], s_dn)
        plan(k, x_own.at[k], x_sib.at[k], sib_recv.at[k, 0], sib)
        plan(k, g_own.at[k], g_sib.at[k], sib_recv.at[k, 1], sib)
    assert count[0] == N_SEND

    def arrive(k):
        if k:
            if ORDER[k][1] == 2 or ORDER[k] == (2, 0):
                for t in range(2):
                    remote(x_own.at[k, t], x_own.at[k, t], ag_send.at[0], ag_recv.at[k, t], sib).wait_recv()
            else:
                remote(x_own.at[k], x_own.at[k], ag_send.at[0], ag_recv.at[k, 0], sib).wait_recv()
            remote(g_own.at[k], g_own.at[k], ag_send.at[0], ag_grecv.at[k], sib).wait_recv()
        for make in sends[k] + (sends["late"] if ORDER[k] == (2, 0) else []):
            make().start()

    def to_sibling(k):
        return (remote(x_sib.at[k], q_buf.at[k], rq_send.at[k, 0], rq_recv.at[k, 0], sib),
                remote(pg_sib.at[k], qg_buf.at[k], rq_send.at[k, 1], rq_recv.at[k, 1], sib))

    def add_sibling(k):
        for c in to_sibling(k):
            c.wait_recv()
        part[k] = part[k] + q_buf[k]
        pg_own[k] = pg_own[k] + qg_buf[k]

    def s_first(df):
        k = SLOT[(df, 2)]
        return (remote(part.at[k, 0], r1.at[df, 0], s1_send.at[df, 0], s1_recv.at[df, 0], s_up),
                remote(part.at[k, 1], r1.at[df, 1], s1_send.at[df, 1], s1_recv.at[df, 1], s_dn),
                remote(pg_own.at[k], r1g.at[df], s1_send.at[df, 2], s1_recv.at[df, 2], s_up))

    def s_second(df, i):
        k = SLOT[(df, (1, 3)[i])]
        dev = (s_up, s_dn)[i]
        return (remote(pg_own.at[k], r2g.at[df, i], s2_send.at[df, i, 1], s2_recv.at[df, i, 1], dev),
                remote(part.at[k], r2.at[df, i], s2_send.at[df, i, 0], s2_recv.at[df, i, 0], dev))

    def add_into(k, t, block):
        part[k, t] = part[k, t] + block[...]

    def send_second(df):
        for c in s_first(df):
            c.wait_recv()
        k = SLOT[(df, 1)]
        add_into(k, 0, r1.at[df, 0])
        pg_own[k] = pg_own[k] + r1g[df]
        add_into(SLOT[(df, 3)], 1, r1.at[df, 1])
        for i in range(2):
            for c in s_second(df, i):
                c.start()

    row = lax.broadcasted_iota(jnp.int32, (n_exp, loc), 0)
    col = lax.broadcasted_iota(jnp.int32, (n_exp, loc), 1)
    pick = jnp.where(row == ep * n_loc + lax.div(col, width), 1.0, 0.0).astype(BF16)
    pick3 = jnp.concatenate([pick] * 3, axis=0)
    ones = jnp.ones((16, 2 * n_tok), BF16)

    def widen(g):
        hi = g.astype(BF16)
        rest = g - hi.astype(F32)
        mid = rest.astype(BF16)
        low = (rest - mid.astype(F32)).astype(BF16)
        return lax.dot_general(jnp.concatenate([hi, mid, low], axis=0), pick3, (((0,), (0,)), ((), ())), preferred_element_type=F32)

    def compute(k):
        h = jnp.concatenate([x_own[k, 0], x_sib[k, 0]], axis=0)
        dy = jnp.concatenate([x_own[k, 1], x_sib[k, 1]], axis=0)
        gate = widen(jnp.concatenate([g_own[k], g_sib[k]], axis=1))
        both = jnp.dot(h, wgu[...], preferred_element_type=F32)
        g_pre = both[:, :loc]
        u_pre = both[:, loc:]
        d_raw = dot_nt(dy, wd[...])
        used = gate != 0.0
        sig = 0.5 * jnp.tanh(0.5 * g_pre) + 0.5
        silu = g_pre * sig
        act = (silu * u_pre).astype(BF16).astype(F32)
        act_g = jnp.where(used, gate * act, 0.0).astype(BF16)
        prod = jnp.where(used, act * d_raw, 0.0)
        d_act = gate * d_raw
        d_g = jnp.where(used, d_act * u_pre * (sig + silu * (1.0 - sig)), 0.0).astype(BF16)
        d_u = jnp.where(used, d_act * silu, 0.0).astype(BF16)
        d_gu = jnp.concatenate([d_g, d_u], axis=1)
        prod_hi = prod.astype(BF16)
        prod_lo = (prod - prod_hi.astype(F32)).astype(BF16)
        dgate = dot_nt(pick, prod_hi) + dot_nt(pick, prod_lo)
        pg_own[k] = dgate[:, :n_tok]
        pg_sib[k] = dgate[:, n_tok:]
        acc_gu[...] += jnp.dot(h.T, d_gu, preferred_element_type=F32)
        acc_d[...] += jnp.dot(jnp.concatenate([act_g.T, ones], axis=0), dy, preferred_element_type=F32)
        y = jnp.dot(act_g, wd[...], preferred_element_type=F32).astype(BF16)
        part[k, 0] = y[:n_tok]
        x_sib[k, 0] = y[n_tok:]
        dh = dot_nt(d_gu, wgu[...]).astype(BF16)
        part[k, 1] = dh[:n_tok]
        x_sib[k, 1] = dh[n_tok:]

    arrive(0)
    acc_gu[...] = jnp.zeros_like(acc_gu)
    acc_d[...] = jnp.zeros_like(acc_d)
    for c in loads:
        c.wait()

    def step(k, carry):
        for j, places in ARRIVALS.items():
            @pl.when(k == j)
            def _():
                if j == 1:
                    for make in sends["own"]:
                        make().start()
                for place in places:
                    arrive(SLOT[place])
        remote(x_own.at[k], x_sib.at[k], ag_send.at[0], sib_recv.at[k, 0], sib).wait_recv()
        remote(g_own.at[k], g_sib.at[k], ag_send.at[0], sib_recv.at[k, 1], sib).wait_recv()
        compute(k)
        for c in to_sibling(k):
            c.start()

        @pl.when(k >= LAG)
        def _():
            add_sibling(k - LAG)
        for j, df in FIRST_AT.items():
            @pl.when(k == j)
            def _():
                for c in s_first(df):
                    c.start()
        for j, df in SECOND_AT.items():
            @pl.when(k == j)
            def _():
                send_second(df)
        return carry

    lax.fori_loop(0, N_SLOT, step, 0)

    send_second(3)

    stores = []
    for e in range(n_loc):
        cols = pl.ds(e * width, width)
        stores.append(pltpu.make_async_copy(acc_gu.at[:, cols], dwg_ref.at[e], load_sem.at[len(stores)]))
        stores.append(pltpu.make_async_copy(acc_gu.at[:, pl.ds(loc + e * width, width)], dwu_ref.at[e], load_sem.at[len(stores)]))
        stores.append(pltpu.make_async_copy(acc_d.at[cols], dwd_ref.at[e], load_sem.at[len(stores)]))
    for c in stores:
        c.start()
    dbias_ref[...] = acc_d[loc:loc + 1]
    for j in range(N_SLOT - LAG, N_SLOT):
        add_sibling(j)

    k2, k1, k3 = SLOT[(2, 0)], SLOT[(1, 0)], SLOT[(3, 0)]

    def wait_second(df):
        for i in range(2):
            for c in s_second(df, i):
                c.wait_recv()
        pg_own[SLOT[(df, 0)]] = pg_own[SLOT[(df, 0)]] + r2g[df, 0] + r2g[df, 1]

    def total(k, df, t):
        return part[k, t].astype(F32) + r2[df, 0, t].astype(F32) + r2[df, 1, t].astype(F32)

    f_first = (remote(pg_own.at[k2], r3g, f1_send.at[2], f1_recv.at[2], f_up),
               remote(part.at[k2, 0], r3.at[0], f1_send.at[0], f1_recv.at[0], f_up),
               remote(part.at[k2, 1], r3.at[1], f1_send.at[1], f1_recv.at[1], f_dn))
    f_second = (remote(pg_own.at[k1], r4g.at[0], f2_send.at[0], f2_recv.at[0], f_up),
                remote(pg_own.at[k3], r4g.at[1], f2_send.at[1], f2_recv.at[1], f_dn),
                remote(part.at[k1, 1], r4.at[0, 1], f2_send.at[2], f2_recv.at[2], f_up),
                remote(part.at[k3, 1], r4.at[1, 1], f2_send.at[3], f2_recv.at[3], f_dn),
                remote(part.at[k1, 0], r4.at[0, 0], f2_send.at[4], f2_recv.at[4], f_up),
                remote(part.at[k3, 0], r4.at[1, 0], f2_send.at[5], f2_recv.at[5], f_dn))
    for df, k in ((2, k2), (1, k1), (3, k3)):
        wait_second(df)
        part[k, 0] = total(k, df, 0).astype(BF16)
        part[k, 1] = total(k, df, 1).astype(BF16)
        if df == 2:
            for c in f_first:
                c.start()
        if df == 1:
            f_first[0].wait_recv()
            pg_own[k1] = pg_own[k1] + r3g[...]
            f_second[0].start()
            f_second[2].start()
            f_first[1].wait_recv()
            add_into(k1, 0, r3.at[0])
    f_second[1].start()
    f_first[2].wait_recv()
    add_into(k3, 1, r3.at[1])
    f_second[3].start()

    gates = g_own[0]
    chosen = chosen_mask()
    x, inv_rms, normed = normalised()
    wait_second(0)
    for c in f_second[:2]:
        c.wait_recv()
    d_gates = jnp.where(chosen, pg_own[0] + r4g[0] + r4g[1], 0.0)
    d_logits = gates * (d_gates - jnp.sum(gates * d_gates, axis=0, keepdims=True))
    dl_buf[0, 0] = d_logits
    s_dl = [remote(dl_buf.at[0, 0], dl_buf.at[0, to], e_send.at[i], e_recv.at[i], dev) for i, (to, dev) in enumerate(((3, s_up), (1, s_dn), (2, s_op)))]
    f_dl = [remote(dl_buf.at[0], dl_buf.at[to], e_send.at[3 + i], e_recv.at[3 + i], dev) for i, (to, dev) in enumerate(((3, f_up), (1, f_dn), (2, f_op)))]
    for c in s_dl:
        c.start()
    dh_router = lax.dot_general(d_logits, router_ref[...].astype(F32), (((0,), (0,)), ((), ())), precision=lax.Precision.HIGHEST, preferred_element_type=F32)
    for c in s_dl:
        c.wait_recv()
    for c in f_dl:
        c.start()
    f_second[4].start()
    f_second[5].start()

    for c in f_second[2:4]:
        c.wait_recv()
    dh_total = total(0, 0, 1) + r4[0, 1].astype(F32) + r4[1, 1].astype(F32) + dh_router
    gn_buf[0] = jnp.sum(dh_total * normed, axis=0, keepdims=True)

    def exchange(base, group, first_sem):
        return [remote(gn_buf.at[base], gn_buf.at[base + 1 + i], e_send.at[first_sem + i], e_recv.at[first_sem + i], dev) for i, dev in enumerate(group)]

    def gathered(base, copies):
        for c in copies:
            c.wait_recv()
        summed = gn_buf[base]
        for i in range(len(copies)):
            summed = summed + gn_buf[base + 1 + i]
        return summed

    gn_sib = exchange(0, (sib,), 7)
    for c in gn_sib:
        c.start()
    d_norm = dh_total * gain
    dx_ref[...] = (dy_ref[...].astype(F32) + inv_rms * (d_norm - normed * jnp.mean(d_norm * normed, axis=-1, keepdims=True))).astype(BF16)
    gn_buf[2] = gathered(0, gn_sib)
    gn_s = exchange(2, (s_up, s_dn, s_op), 8)
    for c in gn_s:
        c.start()
    d_router = jnp.zeros((n_exp, d_model), F32)
    for c in f_dl:
        c.wait_recv()
    for k, (df, ds) in enumerate(ORDER):
        dl = dl_buf[df, ds]
        dl_hi = dl.astype(BF16)
        dl_lo = (dl - dl_hi.astype(F32)).astype(BF16)
        prods = jnp.dot(jnp.concatenate([dl_hi, dl_lo], axis=0), x_own[k, 0], preferred_element_type=F32)
        d_router = d_router + (prods[:n_exp] + prods[n_exp:])
        if k == 3:
            gn_buf[6] = gathered(2, gn_s)
            gn_f = exchange(6, (f_up, f_dn, f_op), 11)
            for c in gn_f:
                c.start()
    dr_buf[0] = d_router
    sib_dr = remote(dr_buf.at[0], dr_buf.at[1], e_send.at[6], e_recv.at[6], sib)
    sib_dr.start()
    for c in f_second[4:]:
        c.wait_recv()
    y_moe = total(0, 0, 0) + r4[0, 0].astype(F32) + r4[1, 0].astype(F32)
    y_ref[...] = (x + (y_moe + bias_ref[...].astype(F32).reshape(1, d_model))).astype(BF16)
    dgain_ref[...] = gathered(6, gn_f)
    sib_dr.wait_recv()
    drouter_ref[...] = dr_buf[0] + dr_buf[1]

    for c in f_dl + s_dl + gn_sib + gn_s + gn_f + [sib_dr]:
        c.wait_send()
    for c in stores:
        c.wait()
    for made in sends.values():
        for make in made:
            make().wait_send()
    for k in range(N_SLOT):
        for c in to_sibling(k):
            c.wait_send()
    for df in range(4):
        for c in s_first(df):
            c.wait_send()
        for i in range(2):
            for c in s_second(df, i):
                c.wait_send()
    for c in f_first + f_second:
        c.wait_send()


def moe(x, dy, idx_t, gain, bias, router_t, w_gate, w_up, w_down):
    n_tok, d_model = x.shape
    n_loc, _, width = w_gate.shape
    n_exp = router_t.shape[0]
    loc = n_loc * width
    vmem = pl.BlockSpec(memory_space=pltpu.VMEM)
    hbm = pl.BlockSpec(memory_space=pl.ANY)
    block = (2, n_tok, d_model)
    small = (n_exp, n_tok)
    dma = pltpu.SemaphoreType.DMA
    scratch = [
        pltpu.VMEM((N_SLOT, *block), BF16), pltpu.VMEM((N_SLOT, *block), BF16), pltpu.VMEM((N_SLOT, *block), BF16),
        pltpu.VMEM((N_SLOT, *small), F32), pltpu.VMEM((N_SLOT, *small), F32),
        pltpu.VMEM((N_SLOT, *small), F32), pltpu.VMEM((N_SLOT, *small), F32),
        pltpu.VMEM((N_SLOT, *block), BF16), pltpu.VMEM((N_SLOT, *small), F32),
        pltpu.VMEM((4, *block), BF16), pltpu.VMEM((4, *small), F32),
        pltpu.VMEM((4, 2, *block), BF16), pltpu.VMEM((4, 2, *small), F32),
        pltpu.VMEM(block, BF16), pltpu.VMEM(small, F32),
        pltpu.VMEM((2, *block), BF16), pltpu.VMEM((2, *small), F32),
        pltpu.VMEM((4, 4, *small), F32), pltpu.VMEM((2, n_exp, d_model), F32), pltpu.VMEM((10, 1, d_model), F32),
        pltpu.VMEM((d_model, 2 * loc), BF16), pltpu.VMEM((loc, d_model), BF16),
        pltpu.VMEM((d_model, 2 * loc), F32), pltpu.VMEM((loc + 16, d_model), F32),
        dma((3 * n_loc,)), dma((N_SEND,)), dma((N_SLOT, 2)), dma((N_SLOT,)), dma((N_SLOT, 2)),
        dma((N_SLOT, 2)), dma((N_SLOT, 2)), dma((4, 3)), dma((4, 3)), dma((4, 2, 2)), dma((4, 2, 2)),
        dma((3,)), dma((3,)), dma((6,)), dma((6,)), dma((14,)), dma((14,)),
    ]
    out_shape = (
        jax.ShapeDtypeStruct((n_tok, d_model), BF16), jax.ShapeDtypeStruct((n_tok, d_model), BF16),
        jax.ShapeDtypeStruct((1, d_model), F32), jax.ShapeDtypeStruct((n_exp, d_model), F32), jax.ShapeDtypeStruct((1, d_model), F32),
        jax.ShapeDtypeStruct(w_gate.shape, F32), jax.ShapeDtypeStruct(w_up.shape, F32), jax.ShapeDtypeStruct(w_down.shape, F32),
    )
    return pl.pallas_call(
        moe_kernel, name="moe", out_shape=out_shape,
        in_specs=[vmem] * 6 + [hbm] * 3, out_specs=(vmem,) * 5 + (hbm,) * 3,
        scratch_shapes=scratch,
        compiler_params=pltpu.CompilerParams(collective_id=0, has_side_effects=True, vmem_limit_bytes=67_043_328),
    )(x, dy, idx_t, gain, bias, router_t, w_gate, w_up, w_down)


def write_out(*refs):
    n = len(refs) // 3
    sources, results, rooms, sems = refs[:n], refs[n:2 * n], refs[2 * n:3 * n], refs[3 * n]
    pieces = []
    for i in range(n):
        for j in range(sources[i].shape[0] if len(sources[i].shape) == 3 else 1):
            at = (lambda r, j=j: r.at[j]) if len(sources[i].shape) == 3 else (lambda r: r)
            m = len(pieces)
            pieces.append((pltpu.make_async_copy(at(sources[i]), at(rooms[i]), sems.at[m, 0]),
                           pltpu.make_async_copy(at(rooms[i]), at(results[i]), sems.at[m, 1])))
    for load, _ in pieces:
        load.start()
    for load, store in pieces:
        load.wait()
        store.start()
    for _, store in pieces:
        store.wait()


def finish(*arrays):
    hbm = pl.BlockSpec(memory_space=pl.ANY)
    n_pieces = sum(a.shape[0] if a.ndim == 3 else 1 for a in arrays)
    return pl.pallas_call(
        write_out, name="finish", out_shape=tuple(jax.ShapeDtypeStruct(a.shape, a.dtype) for a in arrays),
        in_specs=[hbm] * len(arrays), out_specs=(hbm,) * len(arrays),
        scratch_shapes=[pltpu.VMEM(a.shape, a.dtype) for a in arrays] + [pltpu.SemaphoreType.DMA((n_pieces, 2))],
        compiler_params=pltpu.CompilerParams(vmem_limit_bytes=67_043_328),
    )(*arrays)


def solution(mesh):
    tok_spec = P(("dp", "ep", "tp"), None)
    wide_spec = P("ep", None, "tp")
    down_spec = P("ep", "tp", None)
    grad_wide = P(("dp", "ep"), None, "tp")
    grad_down = P(("dp", "ep"), "tp", None)

    def device_step(x_in, norm_gain, w_router, expert_idx, w_gate, w_up, w_down, out_bias, dy_out):
        y_out, dx_in, d_gain, d_router_t, d_bias, d_gate, d_up, d_down = moe(
            x_in, dy_out, expert_idx.T, norm_gain, out_bias, w_router.T, w_gate, w_up, w_down)
        y_out, dx_in, d_gain, d_router_t, d_gate, d_up, d_down, d_bias = finish(y_out, dx_in, d_gain, d_router_t, d_gate, d_up, d_down, d_bias)
        return y_out, dx_in, d_gain[0], d_router_t.T, d_gate, d_up, d_down, d_bias[0]

    return jax.shard_map(device_step, mesh=mesh, in_specs=(tok_spec, P(None), P(None, None), tok_spec, wide_spec, wide_spec, down_spec, P(None), tok_spec), out_specs=(tok_spec, tok_spec, P("dp"), P("dp", None), grad_wide, grad_wide, grad_down, P("dp")), check_vma=False)
```
